32 devices in a mesh: dp: 16 (over z, y, x), mp: 2 (over core).
Axes of the slice: x: 2, y: 2, z: 4, core: 2. Of those that a mesh axis runs over, the one named last changes fastest.
Arguments:
- patches: bfloat16 [8192, 3200], P(('dp', 'mp')), may hold values from -120 to 120
- ln_gain: bfloat16 [3200], replicated, may hold values from 0.099609375 to 1.8984375
- ln_bias: bfloat16 [3200], replicated, may hold values from -3 to 3
- w_proj: bfloat16 [3200, 4096], P(None, 'mp'), may hold values from -0.109375 to 0.109375
- proj_bias: bfloat16 [4096], P('mp'), may hold values from -3 to 3
- rms_gain: bfloat16 [4096], replicated, may hold values from 0.099609375 to 1.8984375
- w_qkv: bfloat16 [4096, 3072], P(None, 'mp'), may hold values from -4 to 4
- image_counts: int32 [64, 8], replicated, may hold values from 1 to 16, as said below
- source_shift: int32 [32], replicated, may hold values from 0 to 15, as said below
Outputs:
- attended: bfloat16 [8192, 2048], P('dp', 'mp')
The draws below stay inside these ranges and needn't reach their ends.
Inputs may be any that keep to these rules, and one draw needn't show every extreme that they name: `image_counts`: row g holds the counts of the 8 images of tile g. In every draw all images of the tiles of some dp index hold 16 tokens. No value stands more than 2 times in source_shift, and some value stands exactly 2 times.
All inputs are finite; a program needn't handle non-finite values.
Results may differ from the reference program's by a relative error of at most 0.012.
Values may be sent and summed in bfloat16 or wider, within the bound.
A program may use at most 128 MiB of HBM per device.

```python
import math
import jax
import jax.numpy as jnp
from jax import lax

D_VIT = 3200
MODEL_WIDTH = 4096
HEAD_SIZE = 128
TILE = 128
IMG_TILE = 8
TOK_DEV = 512
QUERY_PER_KEY = 4
TILES_DEV = 4
IMG_DEV = 32
IMG_MAX = 16
TOKENS = 8192
NTILES = 64
QKV_COLS = 3072
OUT_COLS = 2048
N_DP = 16


def draw_patches(key, part):
    base_key, row_key, col_key = jax.random.split(key, 3)
    row_scale = jnp.exp(jax.random.uniform(row_key, (TOKENS, 1), jnp.float32, 0.0, math.log(10.0)))
    col_scale = jnp.exp(jax.random.uniform(col_key, (1, D_VIT), jnp.float32, math.log(0.3), math.log(3.0)))
    base_values = jax.random.normal(base_key, (TOKENS, D_VIT), jnp.float32)
    return (jnp.clip(base_values, -4.0, 4.0) * row_scale * col_scale).astype(jnp.bfloat16)


def draw_w_qkv(key, part):
    base_key = jax.random.fold_in(key, 0)
    base_values = jnp.clip(jax.random.normal(base_key, (MODEL_WIDTH, QKV_COLS), jnp.float32), -5.0, 5.0) / math.sqrt(MODEL_WIDTH)
    return jnp.clip(base_values, -4.0, 4.0).astype(jnp.bfloat16)


def draw_image_counts(key, part):
    count_key, full_key = jax.random.split(key)
    counts = jax.random.randint(count_key, (NTILES, IMG_TILE), 1, IMG_MAX + 1, dtype=jnp.int32)
    full_device = jax.random.randint(full_key, (), 0, N_DP, dtype=jnp.int32)
    owner_dev = jnp.arange(NTILES, dtype=jnp.int32) // TILES_DEV
    return jnp.where((owner_dev == full_device)[:, None], IMG_MAX, counts).astype(jnp.int32)


def draw_source_shift(key, part):
    cycle_key, order_key = jax.random.split(key)
    random_rank = jax.random.permutation(cycle_key, N_DP).astype(jnp.int32)
    values_all = jnp.arange(N_DP, dtype=jnp.int32)
    scores = jnp.where(values_all == N_DP // 2, -3, jnp.where(values_all == N_DP - 1, -2, jnp.where(values_all == 1, -1, random_rank))).astype(jnp.int32)
    cycle_order = jnp.argsort(scores, stable=True).astype(jnp.int32)
    slot_order = jax.random.permutation(order_key, IMG_DEV).astype(jnp.int32)
    return cycle_order[slot_order % N_DP].astype(jnp.int32)


def shard_levels(stream_key, shape, shards, least, top_value):
    loudness = 1.0
    for axis_at, blocks in shards:
        heights = jax.random.uniform(jax.random.fold_in(jax.random.fold_in(stream_key, 6), axis_at), (blocks,), jnp.float32, least / len(shards), top_value / len(shards))
        loudness = loudness * jnp.repeat(jnp.exp(heights), shape[axis_at] // blocks).reshape((-1,) + (1,) * (len(shape) - 1 - axis_at))
    return loudness


def scatter_about(stream_key, dims, spread, most, cuts=(), kind=jnp.bfloat16):
    drawn = spread * jax.random.normal(stream_key, dims, jnp.float32)
    if cuts:
        drawn = drawn * shard_levels(stream_key, dims, cuts, -0.22, 0.18)
    return jnp.clip(drawn, -most, most).astype(kind)


def setup_inputs(seed: int = 0) -> dict:
    key_list = jax.random.split(jax.random.key(seed), 10)
    return {
        "patches": draw_patches(jax.random.fold_in(key_list[9], 71), 0),
        "ln_gain": jnp.clip(1.0 + 0.18 * jax.random.normal(key_list[1], (D_VIT,), jnp.float32), 0.099609375, 1.8984375).astype(jnp.bfloat16),
        "ln_bias": scatter_about(key_list[2], (D_VIT,), 0.5, 3.0),
        "w_proj": scatter_about(key_list[3], (D_VIT, MODEL_WIDTH), D_VIT ** -0.5, 0.109375, ((1, 2),)),
        "proj_bias": scatter_about(key_list[4], (MODEL_WIDTH,), 0.5, 3.0, ((0, 2),)),
        "rms_gain": jnp.clip(1.0 + 0.18 * jax.random.normal(key_list[5], (MODEL_WIDTH,), jnp.float32), 0.099609375, 1.8984375).astype(jnp.bfloat16),
        "w_qkv": draw_w_qkv(jax.random.fold_in(key_list[9], 71), 0),
        "image_counts": draw_image_counts(jax.random.fold_in(key_list[9], 71), 0),
        "source_shift": draw_source_shift(jax.random.fold_in(key_list[9], 71), 0),
    }


norm_epsilon = 1e-05
rms_epsilon = 1e-05
rotary_base = 500000.0

def routing(image_counts, source_shift):
    per_dest = image_counts.reshape(N_DP, IMG_DEV)
    senders = jnp.arange(N_DP, dtype=jnp.int32)
    dest_of = jnp.mod(senders[:, None] - source_shift[None, :], N_DP).astype(jnp.int32)
    sent_counts = jnp.take_along_axis(per_dest, dest_of, axis=0).astype(jnp.int32)
    starts = (jnp.cumsum(sent_counts, axis=1) - sent_counts).astype(jnp.int32)
    slot_ends = jnp.cumsum(image_counts, axis=1).astype(jnp.int32)
    offsets = (slot_ends - image_counts).astype(jnp.int32)
    position = jnp.arange(TILE, dtype=jnp.int32)
    slot_index = lax.optimization_barrier(jnp.sum((position[None, :, None] >= slot_ends[:, None, :]).astype(jnp.int32), axis=2)).astype(jnp.int32)
    live_rows = slot_index < IMG_TILE
    clipped = jnp.minimum(slot_index, IMG_TILE - 1).astype(jnp.int32)
    inside_tile = position[None, :] - jnp.take_along_axis(offsets, clipped, axis=1)
    tile_count = jnp.arange(NTILES, dtype=jnp.int32)
    owner_dev = tile_count // TILES_DEV
    image_k = ((tile_count % TILES_DEV)[:, None] * IMG_TILE + clipped).astype(jnp.int32)
    sender = jnp.mod(owner_dev[:, None] + source_shift[image_k], N_DP).astype(jnp.int32)
    source_row = sender * TOK_DEV + starts[sender, image_k] + inside_tile
    source_row = jnp.where(live_rows, source_row, 0).astype(jnp.int32)
    return (source_row.reshape(-1), live_rows.reshape(-1), slot_index.reshape(-1))

def layer_norm(row_block, gain_vec, bias_vec):
    values = row_block.astype(jnp.float32)
    row_mean = lax.optimization_barrier(jnp.mean(values, axis=-1, keepdims=True))
    centred = values - row_mean
    row_var = lax.optimization_barrier(jnp.mean(centred * centred, axis=-1, keepdims=True))
    scaled = centred * lax.rsqrt(row_var + norm_epsilon) * gain_vec.astype(jnp.float32)
    return (scaled + bias_vec.astype(jnp.float32)).astype(jnp.bfloat16)

def rotary(values, cos_table, sine_table):
    half_width = values.shape[-1] // 2
    turned = jnp.concatenate([-values[..., half_width:], values[..., :half_width]], axis=-1)
    return values * cos_table + turned * sine_table

def attend(queries, key_rows, value_rows, segment):
    tile_count = queries.shape[0] // TILE
    groups = queries.shape[1]
    query_f = queries.reshape(tile_count, TILE, groups, QUERY_PER_KEY, HEAD_SIZE).astype(jnp.float32)
    key_f = key_rows.reshape(tile_count, TILE, groups, HEAD_SIZE).astype(jnp.float32)
    value_f = value_rows.reshape(tile_count, TILE, groups, HEAD_SIZE).astype(jnp.float32)
    scores = jnp.einsum('tqhgd,tkhd->thgqk', query_f, key_f) * HEAD_SIZE ** (-0.5)
    segments = segment.reshape(tile_count, TILE)
    position = jnp.arange(TILE, dtype=jnp.int32)
    allowed = (position[None, :, None] >= position[None, None, :]) & (segments[:, :, None] == segments[:, None, :])
    scores = jnp.where(allowed[:, None, None], scores, -1e+30)
    row_max = lax.optimization_barrier(jnp.max(scores, axis=-1, keepdims=True))
    weights = jnp.exp(scores - row_max)
    probabilities = (weights / lax.optimization_barrier(jnp.sum(weights, axis=-1, keepdims=True))).astype(jnp.bfloat16)
    attended = jnp.einsum('thgqk,tkhd->tqhgd', probabilities.astype(jnp.float32), value_f)
    return attended.reshape(tile_count * TILE, groups * QUERY_PER_KEY * HEAD_SIZE)

def finish(hidden, live_flat, segment, rms_gain, w_qkv):
    row_total = hidden.shape[0]
    widened = hidden.astype(jnp.float32)
    mean_square = lax.optimization_barrier(jnp.mean(widened * widened, axis=-1, keepdims=True))
    rms_normed = (widened * lax.rsqrt(mean_square + rms_epsilon) * rms_gain.astype(jnp.float32)).astype(jnp.bfloat16)
    projections = jnp.dot(rms_normed, w_qkv, preferred_element_type=jnp.float32)
    groups = w_qkv.shape[1] // ((QUERY_PER_KEY + 2) * HEAD_SIZE)
    projections = projections.reshape(row_total, groups, QUERY_PER_KEY + 2, HEAD_SIZE)
    position = (jnp.arange(row_total, dtype=jnp.int32) % TILE).astype(jnp.float32)
    frequency = rotary_base ** (-(jnp.arange(HEAD_SIZE // 2, dtype=jnp.float32) * (2.0 / HEAD_SIZE)))
    angles = position[:, None] * frequency[None, :]
    cos_table = jnp.concatenate([jnp.cos(angles), jnp.cos(angles)], axis=-1)[:, None, None, :]
    sine_table = jnp.concatenate([jnp.sin(angles), jnp.sin(angles)], axis=-1)[:, None, None, :]
    queries = rotary(projections[:, :, :QUERY_PER_KEY], cos_table, sine_table).astype(jnp.bfloat16)
    key_rows = rotary(projections[:, :, QUERY_PER_KEY], cos_table[:, :, 0], sine_table[:, :, 0]).astype(jnp.bfloat16)
    value_rows = projections[:, :, QUERY_PER_KEY + 1].astype(jnp.bfloat16)
    attended = attend(queries, key_rows, value_rows, segment).astype(jnp.bfloat16)
    return jnp.where(live_flat[:, None], attended, jnp.zeros_like(attended))

def reference(patches, ln_gain, ln_bias, w_proj, proj_bias, rms_gain, w_qkv, image_counts, source_shift):
    source_row, live_rows, slot_index = routing(image_counts, source_shift)

    def device_block(device):
        pick_rows = lax.dynamic_slice_in_dim(source_row, device * TOK_DEV, TOK_DEV)
        live_flat = lax.dynamic_slice_in_dim(live_rows, device * TOK_DEV, TOK_DEV)
        segment = lax.dynamic_slice_in_dim(slot_index, device * TOK_DEV, TOK_DEV)
        gathered = jnp.take(patches, pick_rows, axis=0)
        normed = layer_norm(gathered, ln_gain, ln_bias)
        pre_act = jnp.dot(normed, w_proj, preferred_element_type=jnp.float32) + proj_bias.astype(jnp.float32)
        activated = jax.nn.gelu(pre_act, approximate=False)
        hidden = jnp.where(live_flat[:, None], activated, jnp.zeros_like(activated)).astype(jnp.bfloat16)
        return finish(hidden, live_flat, segment, rms_gain, w_qkv)
    blocks = lax.map(device_block, jnp.arange(N_DP, dtype=jnp.int32))
    return blocks.reshape(TOKENS, OUT_COLS)
```

```python
import functools

import jax
import jax.numpy as jnp
import numpy as np
from jax import lax
from jax.experimental import pallas as pl
from jax.experimental.pallas import tpu as pltpu
from jax.sharding import PartitionSpec as P

HEAD_SIZE = 128
TILE = 128
QUERY_PER_KEY = 4
COL_TILE = 256
LANES = 128
PROJECT_ROWS = 512
CHUNK = 256

norm_epsilon = 1e-05
rms_epsilon = 1e-05
rotary_base = 500000.0

F32 = jnp.float32
BF16 = jnp.bfloat16
I32 = jnp.int32
MESH = pl.DeviceIdType.MESH


def shift_order(senders):
    return sorted(range(senders), key=lambda v: (abs(v - senders // 2), v))


def rotary_table(positions):
    frequency = np.float32(rotary_base) ** (
        -(np.arange(HEAD_SIZE // 2, dtype=np.float32) * np.float32(2.0 / HEAD_SIZE))
    )
    angles = np.arange(positions, dtype=np.float32)[:, None] * frequency[None, :].astype(np.float32)
    cos = np.cos(angles.astype(np.float64)).astype(np.float32)
    sin = np.sin(angles.astype(np.float64)).astype(np.float32)
    both = np.stack([np.concatenate([cos, cos], 1), np.concatenate([-sin, sin], 1)], axis=1)
    return both.reshape(2 * positions, HEAD_SIZE)


def gelu(v):
    return 0.5 * v * (1.0 + lax.erf(v * np.float32(0.5**0.5)))


def iota(shape, axis):
    return lax.broadcasted_iota(jnp.int32, shape, axis)


def lane_sum(x):
    return jnp.sum(x, axis=1, keepdims=True)


def row_sum(x):
    return jnp.sum(x, axis=0, keepdims=True)


def kernel(
    senders,
    order,
    ln_gain,
    ln_bias,
    proj_bias,
    rms_gain,
    counts,
    source_shift,
    table,
    patches,
    w_proj,
    w_qkv,
    inbox,
    meta_cols,
    meta_rows,
    raw,
    w1,
    w2,
    normed,
    spread,
    picked,
    hidden,
    squares,
    pre,
    bias,
    proj,
    cos_at,
    sin_at,
    outbox,
    cols_at,
    rows_at,
    plan,
    plan_at,
    raw_sem,
    w1_sem,
    w2_sem,
    plan_sem,
    meta_sem,
    own_sem,
    norm_send,
    norm_recv,
    hid_send,
    hid_recv,
    sq_send,
    sq_recv,
    a2a_send,
    a2a_recv,
):
    me = lax.axis_index("dp")
    core = lax.axis_index("mp")
    peer = 1 - core
    half, d_vit = raw.shape
    rows = 2 * half
    blocks = d_vit // LANES
    box_rows = outbox.shape[0]
    block = box_rows // senders
    images = source_shift.shape[0]
    tiles_dev = rows // TILE
    img_tile = images // tiles_dev
    img_most = TILE // img_tile
    slots = box_rows // img_most
    pair_slots = block // img_most
    half_cols = w_proj.shape[1]
    qkv_cols = w_qkv.shape[1]
    groups = qkv_cols // ((QUERY_PER_KEY + 2) * HEAD_SIZE)
    tiles1 = half_cols // COL_TILE
    pairs = tiles1 // 2
    tiles2 = qkv_cols // COL_TILE
    big = picked.shape[0]
    bigs = box_rows // big
    chunks = box_rows // CHUNK
    part = half // 2

    def raw_copy(i):
        at = pl.ds(i * part, part)
        return pltpu.make_async_copy(patches.at[at], raw.at[at], raw_sem.at[i])

    def w1_copy(j):
        cols = pl.ds(j * 2 * COL_TILE, 2 * COL_TILE)
        return pltpu.make_async_copy(w_proj.at[:, cols], w1.at[:, cols], w1_sem.at[j])

    def w2_copy(j):
        cols = pl.ds(j * 2 * COL_TILE, 2 * COL_TILE)
        return pltpu.make_async_copy(w_qkv.at[:, cols], w2.at[:, cols], w2_sem.at[j])

    for i in range(2):
        raw_copy(i).start()

    barrier = pltpu.get_barrier_semaphore()
    pl.semaphore_signal(barrier, inc=1, device_id={"mp": peer}, device_id_type=MESH)
    for v in range(1, senders):
        pl.semaphore_signal(
            barrier, inc=1, device_id={"dp": lax.rem(me + v, senders)}, device_id_type=MESH
        )

    sq = (images, images)
    k_at, l_at = iota(sq, 0), iota(sq, 1)
    eye = k_at == l_at
    before = l_at < k_at

    def to_row(col):
        return row_sum(jnp.where(eye, col, 0))

    def to_col(row):
        return lane_sum(jnp.where(eye, row, 0))

    tiles_all = counts.shape[1]
    image_counts = counts[...]
    earlier = jnp.zeros((img_tile, tiles_all), I32)
    for j in range(img_tile - 1):
        earlier += jnp.where(iota((img_tile, tiles_all), 0) > j, image_counts[j : j + 1, :], 0)
    counts_by = jnp.concatenate([image_counts] * tiles_dev, axis=0)
    earlier_by = jnp.concatenate([earlier] * tiles_dev, axis=0)
    tile_at = iota((images, tiles_all), 1)
    own_tile = iota((images, 1), 0) // img_tile

    shift_row = source_shift[...].reshape(1, images)
    shift = to_col(shift_row)
    dest = me - shift
    dest = jnp.where(dest < 0, dest + senders, dest)
    place = jnp.zeros((images, 1), I32)
    for v in range(senders):
        place = jnp.where(shift == order[v], v, place)
    there = tile_at == dest * tiles_dev + own_tile
    starts = lane_sum(jnp.where(before, to_row(lane_sum(jnp.where(there, counts_by, 0))), 0))
    far_offset = lane_sum(jnp.where(there, earlier_by, 0))
    rank = lane_sum(jnp.where(before & (shift_row == shift), 1, 0))
    slot = place * pair_slots + rank

    slot_hit = slot == iota((images, LANES), 1)
    plan[0:1, :] = row_sum(jnp.where(slot_hit, starts * blocks, 0))
    plan[1:2, :] = row_sum(jnp.where(slot_hit, far_offset * 2, 0))
    plan_copy = pltpu.make_async_copy(plan, plan_at, plan_sem)
    plan_copy.start()

    gain_f = ln_gain[...].reshape(1, -1).astype(F32)
    bias_f = ln_bias[...].reshape(1, -1).astype(F32)
    bias[0:1, :] = proj_bias[...].reshape(1, -1).astype(F32)
    gains = rms_gain[...].reshape(1, -1).astype(F32)
    bias[1:2, :] = jnp.where(core == 0, gains[:, :half_cols], gains[:, half_cols:])

    def widen(first, values):
        for h in range(2):
            for b in range(blocks):
                at = pl.ds((first + 8 * h) * blocks + b, 8, stride=blocks)
                spread[at, :] = values[8 * h : 8 * h + 8, b * LANES : (b + 1) * LANES]

    def norm_copy(i):
        mine = normed.at[pl.ds(pl.multiple_of(core * half + i * part, part), part)]
        return pltpu.make_async_remote_copy(
            src_ref=mine,
            dst_ref=mine,
            send_sem=norm_send.at[i],
            recv_sem=norm_recv.at[i],
            device_id={"mp": peer},
            device_id_type=MESH,
        )

    for i in range(2):
        raw_copy(i).wait()
        if i == 0:
            for j in range(tiles1 // 2):
                w1_copy(j).start()
            for j in range(tiles2 // 2):
                w2_copy(j).start()

        @pl.loop(0, part // 16, unroll=4)
        def _(r):
            values = raw[pl.ds(pl.multiple_of(i * part + r * 16, 16), 16), :].astype(F32)
            centred = values - jnp.mean(values, axis=-1, keepdims=True)
            variance = jnp.mean(centred * centred, axis=-1, keepdims=True)
            scaled = centred * lax.rsqrt(variance + norm_epsilon) * gain_f + bias_f
            first = pl.multiple_of(core * half + i * part + r * 16, 16)
            normed[pl.ds(first, 16), :] = scaled.astype(BF16)
            widen(first, scaled)

        if i == 0:
            pl.semaphore_wait(barrier, senders)
        norm_copy(i).start()

    spread[rows * blocks :, :] = jnp.zeros((img_most * blocks, LANES), F32)
    squares[core] = jnp.zeros(squares.shape[1:], F32)

    here = tile_at == me * tiles_dev + own_tile
    my_col = lane_sum(jnp.where(here, counts_by, 0))
    my_off = lane_sum(jnp.where(here, earlier_by, 0))
    my_row = to_row(my_col)
    my_off_row = to_row(my_off)
    slot_row = to_row(slot)
    image_row, t_col = iota((TILE, images), 1), iota((TILE, images), 0)
    image_col, t_row = iota((images, TILE), 0), iota((images, TILE), 1)
    lane_at = iota((TILE, LANES), 1)
    for t in range(tiles_dev):
        hit = (image_row // img_tile == t) & (t_col >= my_off_row) & (t_col < my_off_row + my_row)
        box_at = lane_sum(jnp.where(hit, slot_row * img_most + (t_col - my_off_row) + 1, 0)) - 1
        off_at = lane_sum(jnp.where(hit, my_off_row + 1, 0)) - 1
        cols_at[t * TILE : (t + 1) * TILE, :] = jnp.where(lane_at == 0, box_at, off_at)
        hit = (image_col // img_tile == t) & (t_row >= my_off) & (t_row < my_off + my_col)
        rows_at[0:1, t * TILE : (t + 1) * TILE] = row_sum(jnp.where(hit, my_off + 1, 0)) - 1
        rows_at[1:2, t * TILE : (t + 1) * TILE] = row_sum(jnp.where(hit, t_row - my_off + 1, 0)) - 1
    meta = [
        pltpu.make_async_copy(cols_at, meta_cols, meta_sem.at[0]),
        pltpu.make_async_copy(rows_at, meta_rows, meta_sem.at[1]),
    ]
    for copy in meta:
        copy.start()

    plan_copy.wait()

    @pl.loop(0, slots, unroll=4)
    def _(i):
        first = plan_at[1, i]
        for h in range(img_most // 8):
            to = pl.ds(pl.multiple_of(i * img_most + 8 * h, 8), 8)
            cos_at[to, :] = table[pl.ds(first + 16 * h, 8, stride=2), :]
            sin_at[to, :] = table[pl.ds(first + 16 * h + 1, 8, stride=2), :]

    for i in range(2):
        norm_copy(i).wait_recv()

        @pl.loop(0, part // 16, unroll=2)
        def _(r):
            first = pl.multiple_of(peer * half + i * part + r * 16, 16)
            widen(first, normed[pl.ds(first, 16), :].astype(F32))

    def copy_hidden(c, p):
        cols = pl.ds(pl.multiple_of(core * half_cols + p * 2 * COL_TILE, COL_TILE), 2 * COL_TILE)
        ref = hidden.at[pl.ds(c * big, big), cols]
        return pltpu.make_async_remote_copy(
            src_ref=ref,
            dst_ref=ref,
            send_sem=hid_send.at[c * pairs + p],
            recv_sem=hid_recv.at[c * pairs + p],
            device_id={"mp": peer},
            device_id_type=MESH,
        )

    def copy_squares(c):
        ref = squares.at[core, pl.ds(c * big, big)]
        return pltpu.make_async_remote_copy(
            src_ref=ref,
            dst_ref=ref,
            send_sem=sq_send.at[c],
            recv_sem=sq_recv.at[c],
            device_id={"mp": peer},
            device_id_type=MESH,
        )

    def copy_block(o):
        at = pl.ds(o * block, block)
        return pltpu.make_async_remote_copy(
            src_ref=outbox.at[at],
            dst_ref=inbox.at[at],
            send_sem=a2a_send.at[o],
            recv_sem=a2a_recv.at[o],
            device_id={"dp": lax.rem(me + senders - order[o], senders)},
            device_id_type=MESH,
        )

    def own_copy():
        at = pl.ds(box_rows - block, block)
        return pltpu.make_async_copy(outbox.at[at], inbox.at[at], own_sem)

    def columns(j):
        return pl.ds(pl.multiple_of(j * COL_TILE, COL_TILE), COL_TILE)

    def project(c):
        @pl.loop(0, big // img_most, unroll=2)
        def _(i):
            first = plan_at[0, c * (big // img_most) + i]
            to = pl.ds(pl.multiple_of(i * img_most, img_most), img_most)
            for b in range(blocks):
                picked[to, b * LANES : (b + 1) * LANES] = jnp.concatenate(
                    [
                        spread[pl.ds(first + 8 * h * blocks + b, 8, stride=blocks), :]
                        for h in range(img_most // 8)
                    ],
                    axis=0,
                ).astype(BF16)

        if c == 0:
            for j in range(tiles1 // 2):
                w1_copy(j).wait()

        def multiply(j, slot):
            pre[slot] = jnp.dot(picked[...], w1[:, columns(j)], preferred_element_type=F32)

        def activate(j, slot):
            y = gelu(pre[slot] + bias[0:1, columns(j)])
            z = y * y
            total = z[:, :LANES]
            for b in range(1, COL_TILE // LANES):
                total = total + z[:, b * LANES : (b + 1) * LANES]
            squares[core, pl.ds(c * big, big), :] += total
            to = pl.ds(pl.multiple_of(core * half_cols + j * COL_TILE, COL_TILE), COL_TILE)
            hidden[pl.ds(c * big, big), to] = (y * bias[1:2, columns(j)]).astype(BF16)

        multiply(0, 0)

        @pl.loop(0, pairs - 1)
        def _(i):
            multiply(2 * i + 1, 1)
            activate(2 * i, 0)
            multiply(2 * i + 2, 0)
            activate(2 * i + 1, 1)
            copy_hidden(c, i).start()

        multiply(tiles1 - 1, 1)
        activate(tiles1 - 2, 0)
        activate(tiles1 - 1, 1)
        copy_squares(c).start()
        copy_hidden(c, pairs - 1).start()

    wide_at = iota((img_most, QUERY_PER_KEY * TILE), 1)
    causal = iota((img_most, QUERY_PER_KEY * TILE), 0) <= wide_at % img_most
    own_image = (wide_at % TILE) // img_most
    w = HEAD_SIZE

    def qkv(c):
        here = pl.ds(c * CHUNK, CHUNK)
        fresh = c * CHUNK % big == 0
        if c == 0:
            for j in range(tiles2 // 2):
                w2_copy(j).wait()
        if fresh:
            mine = pl.ds(pl.multiple_of(core * half_cols, half_cols), half_cols)
            other = pl.ds(pl.multiple_of(peer * half_cols, half_cols), half_cols)

            @pl.loop(0, tiles2 // 2)
            def _(j):
                cols = pl.ds(pl.multiple_of(j * 2 * COL_TILE, COL_TILE), 2 * COL_TILE)
                proj[:, cols] = jnp.dot(hidden[here, mine], w2[mine, cols], preferred_element_type=F32)

            copy_squares(c * CHUNK // big).wait_recv()
            for p in range(pairs):
                copy_hidden(c * CHUNK // big, p).wait_recv()

            @pl.loop(0, tiles2 // 2)
            def _(j):
                cols = pl.ds(pl.multiple_of(j * 2 * COL_TILE, COL_TILE), 2 * COL_TILE)
                proj[:, cols] += jnp.dot(
                    hidden[here, other], w2[other, cols], preferred_element_type=F32
                )
        else:

            @pl.loop(0, tiles2 // 2)
            def _(j):
                cols = pl.ds(pl.multiple_of(j * 2 * COL_TILE, COL_TILE), 2 * COL_TILE)
                proj[:, cols] = jnp.dot(hidden[here, :], w2[:, cols], preferred_element_type=F32)

    def attend(c):
        for first in range(0, CHUNK, TILE):
            to = pl.ds(c * CHUNK + first, TILE)
            total = lane_sum(squares[0, to, :] + squares[1, to, :])
            scale = lax.rsqrt(total * (1.0 / (2 * half_cols)) + rms_epsilon)
            cos = cos_at[to, :] * scale
            sin = sin_at[to, :] * scale

            def head(h):
                return proj[first : first + TILE, h * w : (h + 1) * w]

            def turned(h):
                v = head(h)
                return (v * cos + pltpu.roll(v, w // 2, 1) * sin).astype(BF16)

            seen = []
            for g in range(groups):
                h0 = g * (QUERY_PER_KEY + 2)
                q = jnp.concatenate([turned(h0 + i) for i in range(QUERY_PER_KEY)], axis=0)
                k = turned(h0 + QUERY_PER_KEY)
                outbox[to, (g + 1) * w : (g + 2) * w] = (head(h0 + QUERY_PER_KEY + 1) * scale).astype(BF16)
                scores = lax.dot_general(
                    k, q, (((1,), (1,)), ((), ())), preferred_element_type=F32
                )
                kept = scores[:img_most]
                for j in range(1, img_tile):
                    kept = jnp.where(own_image == j, scores[j * img_most : (j + 1) * img_most], kept)
                kept = jnp.where(causal, kept * np.float32(HEAD_SIZE ** (-0.5)), -1e30)
                weights = jnp.exp(kept - jnp.max(kept, axis=0, keepdims=True))
                probs = weights / row_sum(weights)
                seen += [probs[:, i * TILE : (i + 1) * TILE] for i in range(QUERY_PER_KEY)]
            outbox[to, :w] = jnp.concatenate(seen, axis=0).T.astype(BF16)
            for o in range((c * CHUNK + first) // block, (c * CHUNK + first + TILE) // block):
                if o < senders - 1:
                    copy_block(o).start()
                else:
                    own_copy().start()

    for c in range(bigs):
        project(c)
    for c in range(chunks):
        qkv(c)
        attend(c)

    for o in range(senders - 1):
        copy_block(o).wait_recv()
    own_copy().wait()
    for copy in meta:
        copy.wait()
    for i in range(2):
        norm_copy(i).wait_send()
    for c in range(bigs):
        copy_squares(c).wait_send()
        for p in range(pairs):
            copy_hidden(c, p).wait_send()
    for o in range(senders - 1):
        copy_block(o).wait_send()


def place_kernel(heads, img_most, meta_cols, meta_rows, box, out, placed, out_sem):
    box_rows = box.shape[0]
    groups = heads // QUERY_PER_KEY
    w = HEAD_SIZE
    tiles = out.shape[0] // TILE

    def out_copy(t):
        at = pl.ds(t * TILE, TILE)
        return pltpu.make_async_copy(placed.at[at], out.at[at], out_sem.at[t])

    key_at = iota((heads * img_most, TILE), 0)
    for t in range(tiles):
        at = slice(t * TILE, (t + 1) * TILE)
        select = jnp.where(iota((TILE, box_rows), 1) == meta_cols[at, 0:1], 1.0, 0.0).astype(BF16)
        got = jnp.dot(select, box[...], preferred_element_type=F32).astype(BF16)
        inside = meta_rows[1:2, at]
        expand = jnp.concatenate(
            [jnp.where(key_at == h * img_most + inside, 1.0, 0.0).astype(BF16) for h in range(heads)],
            axis=1,
        )
        probs = jnp.dot(got[:, : heads * img_most], expand, preferred_element_type=F32)
        same = meta_cols[at, 1:2] == meta_rows[0:1, at]
        for g in range(groups):
            seen = jnp.concatenate(
                [
                    jnp.where(same, probs[:, h * TILE : (h + 1) * TILE], 0.0).astype(BF16)
                    for h in range(g * QUERY_PER_KEY, (g + 1) * QUERY_PER_KEY)
                ],
                axis=0,
            )
            values = got[:, heads * img_most + g * w : heads * img_most + (g + 1) * w]
            attended = jnp.dot(seen, values, preferred_element_type=F32).astype(BF16)
            for i in range(QUERY_PER_KEY):
                a = (g * QUERY_PER_KEY + i) * w
                placed[at, a : a + w] = attended[i * TILE : (i + 1) * TILE]
        out_copy(t).start()
    for t in range(tiles):
        out_copy(t).wait()


def local(
    patches, ln_gain, ln_bias, w_proj, proj_bias, rms_gain, w_qkv, image_counts, source_shift
):
    senders = lax.axis_size("dp")
    order = shift_order(senders)
    half, d_vit = patches.shape
    rows = 2 * half
    half_cols = w_proj.shape[1]
    qkv_cols = w_qkv.shape[1]
    groups = qkv_cols // ((QUERY_PER_KEY + 2) * HEAD_SIZE)
    heads = groups * QUERY_PER_KEY
    out_cols = heads * HEAD_SIZE
    images = source_shift.shape[0]
    img_most = TILE // (images // (rows // TILE))
    pair_slots = (images + senders - 1) // senders
    box_rows = senders * pair_slots * img_most
    box_cols = heads * img_most + groups * HEAD_SIZE
    big = min(PROJECT_ROWS, box_rows)
    bigs = box_rows // big
    pairs = half_cols // COL_TILE // 2
    vmem = pl.BlockSpec(memory_space=pltpu.VMEM)
    hbm = pl.BlockSpec(memory_space=pl.ANY)
    dma = pltpu.SemaphoreType.DMA
    box, cols, lines = pl.pallas_call(
        functools.partial(kernel, senders, order),
        out_shape=[
            jax.ShapeDtypeStruct((box_rows, box_cols), BF16),
            jax.ShapeDtypeStruct((rows, LANES), I32),
            jax.ShapeDtypeStruct((8, rows), I32),
        ],
        in_specs=[vmem] * 7 + [hbm] * 3,
        out_specs=[hbm] * 3,
        scratch_shapes=[
            pltpu.VMEM((half, d_vit), BF16),
            pltpu.VMEM(w_proj.shape, BF16),
            pltpu.VMEM(w_qkv.shape, BF16),
            pltpu.VMEM((rows, d_vit), BF16),
            pltpu.VMEM(((rows + img_most) * (d_vit // LANES), LANES), F32),
            pltpu.VMEM((big, d_vit), BF16),
            pltpu.VMEM((box_rows, 2 * half_cols), BF16),
            pltpu.VMEM((2, box_rows, LANES), F32),
            pltpu.VMEM((2, big, COL_TILE), F32),
            pltpu.VMEM((2, half_cols), F32),
            pltpu.VMEM((CHUNK, qkv_cols), F32),
            pltpu.VMEM((box_rows, HEAD_SIZE), F32),
            pltpu.VMEM((box_rows, HEAD_SIZE), F32),
            pltpu.VMEM((box_rows, box_cols), BF16),
            pltpu.VMEM((rows, LANES), I32),
            pltpu.VMEM((8, rows), I32),
            pltpu.VMEM((8, LANES), I32),
            pltpu.SMEM((8, LANES), I32),
            dma((2,)),
            dma((half_cols // COL_TILE // 2,)),
            dma((qkv_cols // COL_TILE // 2,)),
            dma,
            dma((2,)),
            dma,
            dma((2,)),
            dma((2,)),
            dma((bigs * pairs,)),
            dma((bigs * pairs,)),
            dma((bigs,)),
            dma((bigs,)),
            dma((senders,)),
            dma((senders,)),
        ],
        compiler_params=pltpu.CompilerParams(
            collective_id=0, has_side_effects=True, vmem_limit_bytes=60 * 1024 * 1024
        ),
        name="projector_attention",
    )(
        ln_gain,
        ln_bias,
        proj_bias,
        rms_gain,
        image_counts.T,
        source_shift,
        jnp.asarray(rotary_table(TILE + img_most)),
        patches,
        w_proj,
        w_qkv,
    )
    return pl.pallas_call(
        functools.partial(place_kernel, heads, img_most),
        out_shape=jax.ShapeDtypeStruct((rows, out_cols), BF16),
        in_specs=[vmem] * 3,
        out_specs=hbm,
        scratch_shapes=[pltpu.VMEM((rows, out_cols), BF16), dma((rows // TILE,))],
        name="place",
    )(cols, lines, box)


def solution(mesh):
    in_specs = (
        P(("dp", "mp"), None),
        P(),
        P(),
        P(None, "mp"),
        P("mp"),
        P(),
        P(None, "mp"),
        P(),
        P(),
    )
    out_specs = P("dp", "mp")
    return jax.shard_map(local, mesh=mesh, in_specs=in_specs, out_specs=out_specs, check_vma=False)
```

```python
import functools

import jax
import jax.numpy as jnp
import numpy as np
from jax import lax
from jax.experimental import pallas as pl
from jax.experimental.pallas import tpu as pltpu
from jax.sharding import PartitionSpec as P

HEAD_SIZE = 128
TILE = 128
QUERY_PER_KEY = 4
COL_TILE = 512
LANES = 128
CHUNK = 256

norm_epsilon = 1e-05
rms_epsilon = 1e-05
rotary_base = 500000.0

F32 = jnp.float32
BF16 = jnp.bfloat16
I32 = jnp.int32
MESH = pl.DeviceIdType.MESH


def shift_order(senders):
    return sorted(range(senders), key=lambda v: (abs(v - senders // 2), v))


def rotary_table(positions):
    frequency = np.float32(rotary_base) ** (
        -(np.arange(HEAD_SIZE // 2, dtype=np.float32) * np.float32(2.0 / HEAD_SIZE))
    )
    angles = np.arange(positions, dtype=np.float32)[:, None] * frequency[None, :].astype(np.float32)
    cos = np.cos(angles.astype(np.float64)).astype(np.float32)
    sin = np.sin(angles.astype(np.float64)).astype(np.float32)
    both = np.stack([np.concatenate([cos, cos], 1), np.concatenate([-sin, sin], 1)], axis=1)
    return both.reshape(2 * positions, HEAD_SIZE)


def gelu(v):
    return 0.5 * v * (1.0 + lax.erf(v * np.float32(0.5**0.5)))


def iota(shape, axis):
    return lax.broadcasted_iota(jnp.int32, shape, axis)


def lane_sum(x):
    return jnp.sum(x, axis=1, keepdims=True)


def row_sum(x):
    return jnp.sum(x, axis=0, keepdims=True)


def kernel(
    senders,
    order,
    ln_gain_in,
    ln_bias_in,
    proj_bias_in,
    rms_gain_in,
    counts_in,
    source_shift_in,
    table_in,
    patches,
    w_proj,
    w_qkv,
    box_probs,
    box_values,
    meta_cols,
    meta_rows,
    ln_gain,
    ln_bias,
    proj_bias,
    rms_gain,
    counts,
    source_shift,
    table,
    raw,
    w1,
    w2,
    normed,
    spread,
    picked,
    hidden,
    squares,
    bias,
    proj,
    cos_at,
    sin_at,
    probs_at,
    values_at,
    cols_at,
    rows_at,
    plan,
    plan_at,
    small_sem,
    raw_sem,
    w1_sem,
    w2_sem,
    plan_sem,
    meta_sem,
    norm_send,
    norm_recv,
    hid_send,
    hid_recv,
    sq_send,
    sq_recv,
    probs_send,
    probs_recv,
    values_send,
    values_recv,
):
    me = lax.axis_index("dp")
    core = lax.axis_index("mp")
    peer = 1 - core
    half, d_vit = raw.shape
    rows = 2 * half
    blocks = d_vit // LANES
    box_rows = values_at.shape[0]
    block = box_rows // senders
    images = source_shift.shape[0]
    tiles_dev = rows // TILE
    img_tile = images // tiles_dev
    img_most = TILE // img_tile
    slots = box_rows // img_most
    pair_slots = block // img_most
    half_cols = w_proj.shape[1]
    qkv_cols = w_qkv.shape[1]
    groups = qkv_cols // ((QUERY_PER_KEY + 2) * HEAD_SIZE)
    tiles1 = half_cols // COL_TILE
    qk_group = (QUERY_PER_KEY + 1) * HEAD_SIZE
    qk_cols = groups * qk_group
    chunks = box_rows // CHUNK
    part = 64
    parts = half // part

    def raw_copy(i):
        at = pl.ds(i * part, part)
        return pltpu.make_async_copy(patches.at[at], raw.at[at], raw_sem.at[i])

    def w1_copy(j):
        cols = pl.ds(j * COL_TILE, COL_TILE)
        return pltpu.make_async_copy(w_proj.at[:, cols], w1.at[:, cols], w1_sem.at[j])

    def w2_copy(j):
        g = j // 2
        first = g * (qk_group + HEAD_SIZE)
        if j % 2 == 0:
            source, to, width = first, g * qk_group, qk_group
        else:
            source, to, width = first + qk_group, qk_cols + g * HEAD_SIZE, HEAD_SIZE
        return pltpu.make_async_copy(
            w_qkv.at[:, pl.ds(source, width)], w2.at[:, pl.ds(to, width)], w2_sem.at[j]
        )

    smalls = [
        pltpu.make_async_copy(there, here, small_sem.at[i])
        for i, (there, here) in enumerate(
            [
                (counts_in, counts),
                (source_shift_in, source_shift),
                (ln_gain_in, ln_gain),
                (ln_bias_in, ln_bias),
                (proj_bias_in, proj_bias),
                (rms_gain_in, rms_gain),
                (table_in, table),
            ]
        )
    ]
    for copy in smalls[:2]:
        copy.start()
    for i in range(parts):
        raw_copy(i).start()
    for copy in smalls[2:]:
        copy.start()

    barrier = pltpu.get_barrier_semaphore()
    pl.semaphore_signal(barrier, inc=1, device_id={"mp": peer}, device_id_type=MESH)
    for v in range(1, senders):
        pl.semaphore_signal(
            barrier, inc=1, device_id={"dp": lax.rem(me + v, senders)}, device_id_type=MESH
        )

    for copy in smalls[:2]:
        copy.wait()
    sq = (images, images)
    k_at, l_at = iota(sq, 0), iota(sq, 1)
    eye = k_at == l_at
    before = l_at < k_at

    def to_row(col):
        return row_sum(jnp.where(eye, col, 0))

    def to_col(row):
        return lane_sum(jnp.where(eye, row, 0))

    tiles_all = counts.shape[1]
    image_counts = counts[...]
    earlier = jnp.zeros((img_tile, tiles_all), I32)
    for j in range(img_tile - 1):
        earlier += jnp.where(iota((img_tile, tiles_all), 0) > j, image_counts[j : j + 1, :], 0)
    counts_by = jnp.concatenate([image_counts] * tiles_dev, axis=0)
    earlier_by = jnp.concatenate([earlier] * tiles_dev, axis=0)
    tile_at = iota((images, tiles_all), 1)
    own_tile = iota((images, 1), 0) // img_tile

    shift_row = source_shift[...].reshape(1, images)
    shift = to_col(shift_row)
    dest = me - shift
    dest = jnp.where(dest < 0, dest + senders, dest)
    place = jnp.zeros((images, 1), I32)
    for v in range(senders):
        place = jnp.where(shift == order[v], v, place)
    there = tile_at == dest * tiles_dev + own_tile
    starts = lane_sum(jnp.where(before, to_row(lane_sum(jnp.where(there, counts_by, 0))), 0))
    far_offset = lane_sum(jnp.where(there, earlier_by, 0))
    rank = lane_sum(jnp.where(before & (shift_row == shift), 1, 0))
    slot = place * pair_slots + rank

    slot_hit = slot == iota((images, LANES), 1)
    plan[0:1, :] = row_sum(jnp.where(slot_hit, starts * blocks, 0))
    plan[1:2, :] = row_sum(jnp.where(slot_hit, far_offset * 2, 0))
    plan_copy = pltpu.make_async_copy(plan, plan_at, plan_sem)
    plan_copy.start()

    for copy in smalls[2:]:
        copy.wait()
    gain_f = ln_gain[...].reshape(1, -1).astype(F32)
    bias_f = ln_bias[...].reshape(1, -1).astype(F32)
    bias[0:1, :] = proj_bias[...].reshape(1, -1).astype(F32)
    gains = rms_gain[...].reshape(1, -1).astype(F32)
    bias[1:2, :] = jnp.where(core == 0, gains[:, :half_cols], gains[:, half_cols:])

    def widen(first, values):
        for h in range(2):
            for b in range(blocks):
                at = pl.ds((first + 8 * h) * blocks + b, 8, stride=blocks)
                spread[at, :] = values[8 * h : 8 * h + 8, b * LANES : (b + 1) * LANES]

    def norm_copy(i):
        mine = normed.at[pl.ds(pl.multiple_of(core * half + i * part, part), part)]
        return pltpu.make_async_remote_copy(
            src_ref=mine,
            dst_ref=mine,
            send_sem=norm_send.at[i],
            recv_sem=norm_recv.at[i],
            device_id={"mp": peer},
            device_id_type=MESH,
        )

    for i in range(parts):
        raw_copy(i).wait()
        if i == 0:
            for j in range(tiles1):
                w1_copy(j).start()

        @pl.loop(0, part // 16, unroll=4)
        def _(r):
            values = raw[pl.ds(pl.multiple_of(i * part + r * 16, 16), 16), :].astype(F32)
            centred = values - jnp.mean(values, axis=-1, keepdims=True)
            variance = jnp.mean(centred * centred, axis=-1, keepdims=True)
            scaled = centred * lax.rsqrt(variance + norm_epsilon) * gain_f + bias_f
            first = pl.multiple_of(core * half + i * part + r * 16, 16)
            normed[pl.ds(first, 16), :] = scaled.astype(BF16)
            widen(first, scaled)

        if i == 0:
            pl.semaphore_wait(barrier, senders)
        norm_copy(i).start()

    spread[rows * blocks :, :] = jnp.zeros((img_most * blocks, LANES), F32)

    here = tile_at == me * tiles_dev + own_tile
    my_col = lane_sum(jnp.where(here, counts_by, 0))
    my_off = lane_sum(jnp.where(here, earlier_by, 0))
    my_row = to_row(my_col)
    my_off_row = to_row(my_off)
    slot_row = to_row(slot)
    image_row, t_col = iota((TILE, images), 1), iota((TILE, images), 0)
    image_col, t_row = iota((images, TILE), 0), iota((images, TILE), 1)
    lane_at = iota((TILE, LANES), 1)
    for t in range(tiles_dev):
        hit = (image_row // img_tile == t) & (t_col >= my_off_row) & (t_col < my_off_row + my_row)
        box_at = lane_sum(jnp.where(hit, slot_row * img_most + (t_col - my_off_row) + 1, 0)) - 1
        off_at = lane_sum(jnp.where(hit, my_off_row + 1, 0)) - 1
        cols_at[t * TILE : (t + 1) * TILE, :] = jnp.where(lane_at == 0, box_at, off_at)
        hit = (image_col // img_tile == t) & (t_row >= my_off) & (t_row < my_off + my_col)
        rows_at[0:1, t * TILE : (t + 1) * TILE] = row_sum(jnp.where(hit, my_off + 1, 0)) - 1
        rows_at[1:2, t * TILE : (t + 1) * TILE] = row_sum(jnp.where(hit, t_row - my_off + 1, 0)) - 1
    meta = [
        pltpu.make_async_copy(cols_at, meta_cols, meta_sem.at[0]),
        pltpu.make_async_copy(rows_at, meta_rows, meta_sem.at[1]),
    ]
    for copy in meta:
        copy.start()

    plan_copy.wait()

    @pl.loop(0, slots, unroll=4)
    def _(i):
        first = plan_at[1, i]
        for h in range(img_most // 8):
            to = pl.ds(pl.multiple_of(i * img_most + 8 * h, 8), 8)
            cos_at[to, :] = table[pl.ds(first + 16 * h, 8, stride=2), :]
            sin_at[to, :] = table[pl.ds(first + 16 * h + 1, 8, stride=2), :]

    for i in range(parts):
        norm_copy(i).wait_recv()

        @pl.loop(0, part // 16, unroll=2)
        def _(r):
            first = pl.multiple_of(peer * half + i * part + r * 16, 16)
            widen(first, normed[pl.ds(first, 16), :].astype(F32))

    mine = pl.ds(pl.multiple_of(core * half_cols, half_cols), half_cols)

    def to_peer(ref, send_sem, recv_sem):
        return pltpu.make_async_remote_copy(
            src_ref=ref,
            dst_ref=ref,
            send_sem=send_sem,
            recv_sem=recv_sem,
            device_id={"mp": peer},
            device_id_type=MESH,
        )

    def copy_hidden(c):
        return to_peer(hidden.at[pl.ds(c * CHUNK, CHUNK), mine], hid_send.at[c], hid_recv.at[c])

    def copy_squares(c):
        return to_peer(squares.at[core, pl.ds(c * CHUNK, CHUNK)], sq_send.at[c], sq_recv.at[c])

    def exchange(o, outbox, inbox, send_sem, recv_sem):
        at = pl.ds(o * block, block)
        if o == senders - 1:
            return pltpu.make_async_copy(outbox.at[at], inbox.at[at], send_sem.at[o])
        return pltpu.make_async_remote_copy(
            src_ref=outbox.at[at],
            dst_ref=inbox.at[at],
            send_sem=send_sem.at[o],
            recv_sem=recv_sem.at[o],
            device_id={"dp": lax.rem(me + senders - order[o], senders)},
            device_id_type=MESH,
        )

    def copy_probs(o):
        return exchange(o, probs_at, box_probs, probs_send, probs_recv)

    def copy_values(o):
        return exchange(o, values_at, box_values, values_send, values_recv)


    @pl.loop(0, slots, unroll=2)
    def _(i):
        first = plan_at[0, i]
        to = pl.ds(pl.multiple_of(i * img_most, img_most), img_most)
        for b in range(blocks):
            picked[to, b * LANES : (b + 1) * LANES] = jnp.concatenate(
                [
                    spread[pl.ds(first + 8 * h * blocks + b, 8, stride=blocks), :]
                    for h in range(img_most // 8)
                ],
                axis=0,
            ).astype(BF16)

    def project(c):
        at = pl.ds(c * CHUNK, CHUNK)
        for j in range(tiles1):
            if c == 0 and j % 2 == 0:
                w1_copy(j).wait()
                w1_copy(j + 1).wait()
                if j + 2 == tiles1:
                    for g in range(2 * groups):
                        w2_copy(g).start()
            cols = slice(j * COL_TILE, (j + 1) * COL_TILE)
            pre = jnp.dot(picked[at, :], w1[:, cols], preferred_element_type=F32)
            y = gelu(pre + bias[0:1, cols])
            z = y * y
            total = z[:, :LANES]
            for b in range(1, COL_TILE // LANES):
                total = total + z[:, b * LANES : (b + 1) * LANES]
            if j == 0:
                squares[core, at, :] = total
            else:
                squares[core, at, :] += total
            to = pl.ds(pl.multiple_of(core * half_cols + j * COL_TILE, COL_TILE), COL_TILE)
            hidden[at, to] = (y * bias[1:2, cols]).astype(BF16)
        copy_squares(c).start()
        copy_hidden(c).start()

    wide_at = iota((img_most, QUERY_PER_KEY * TILE), 1)
    causal = iota((img_most, QUERY_PER_KEY * TILE), 0) <= wide_at % img_most
    own_image = (wide_at % TILE) // img_most
    w = HEAD_SIZE

    def product(c, cols):
        return jnp.dot(hidden[pl.ds(c * CHUNK, CHUNK), :], w2[:, cols], preferred_element_type=F32)

    qk_tiles = [slice(f, min(f + COL_TILE, qk_cols)) for f in range(0, qk_cols, COL_TILE)]

    def qk(c, j):
        proj[c % 2, :, qk_tiles[j]] = product(c, qk_tiles[j])

    def values(c):
        at = pl.ds(c * CHUNK, CHUNK)
        copy_squares(c).wait_recv()
        copy_hidden(c).wait_recv()
        if c == 0:
            for j in range(2 * groups):
                w2_copy(j).wait()
        total = lane_sum(squares[0, at, :] + squares[1, at, :])
        scale = lax.rsqrt(total * (1.0 / (2 * half_cols)) + rms_epsilon)
        value_rows = product(c, slice(qk_cols, qkv_cols))
        qk(c, 0)
        values_at[at, :] = (value_rows * scale).astype(BF16)
        cos_at[at, :] *= scale
        sin_at[at, :] *= scale
        for o in range(c * CHUNK // block, (c + 1) * CHUNK // block):
            copy_values(o).start()

    def attend(c, first):
        to = pl.ds(c * CHUNK + first, TILE)
        cos = cos_at[to, :]
        sin = sin_at[to, :]

        def turned(h):
            v = proj[c % 2, first : first + TILE, h * w : (h + 1) * w]
            return (v * cos + pltpu.roll(v, w // 2, 1) * sin).astype(BF16)

        seen = []
        for g in range(groups):
            h0 = g * (QUERY_PER_KEY + 1)
            q = jnp.concatenate([turned(h0 + i) for i in range(QUERY_PER_KEY)], axis=0)
            k = turned(h0 + QUERY_PER_KEY)
            scores = lax.dot_general(
                k, q, (((1,), (1,)), ((), ())), preferred_element_type=F32
            )
            kept = scores[:img_most]
            for j in range(1, img_tile):
                kept = jnp.where(own_image == j, scores[j * img_most : (j + 1) * img_most], kept)
            kept = jnp.where(causal, kept * np.float32(HEAD_SIZE ** (-0.5)), -1e30)
            weights = jnp.exp(kept - jnp.max(kept, axis=0, keepdims=True))
            probs = weights / row_sum(weights)
            seen += [probs[:, i * TILE : (i + 1) * TILE] for i in range(QUERY_PER_KEY)]
        probs_at[to, :] = jnp.concatenate(seen, axis=0).T.astype(BF16)
        for o in range((c * CHUNK + first) // block, (c * CHUNK + first + TILE) // block):
            copy_probs(o).start()

    tiles = CHUNK // TILE
    project(0)
    if chunks > 1:
        project(1)
    values(0)
    for j in range(1, len(qk_tiles)):
        qk(0, j)
    for c in range(chunks):
        if c + 2 < chunks:
            project(c + 2)
        if c + 1 < chunks:
            values(c + 1)
        for j in range(max(tiles, len(qk_tiles))):
            if c + 1 < chunks and j + 1 < len(qk_tiles):
                qk(c + 1, j + 1)
            if j < tiles:
                attend(c, j * TILE)

    for copy in (copy_values, copy_probs):
        for o in range(senders - 1):
            copy(o).wait_recv()
        copy(senders - 1).wait()
    for copy in meta:
        copy.wait()
    for i in range(parts):
        norm_copy(i).wait_send()
    for c in range(chunks):
        copy_squares(c).wait_send()
        copy_hidden(c).wait_send()
    for copy in (copy_values, copy_probs):
        for o in range(senders - 1):
            copy(o).wait_send()


def place_kernel(heads, img_most, *refs):
    cols_in, rows_in, probs_in, values_in, out, meta_cols, meta_rows, box, placed, in_sem, out_sem = refs
    box_rows, prob_cols = probs_in.shape
    loads = [
        pltpu.make_async_copy(there, here, in_sem.at[i])
        for i, (there, here) in enumerate(
            [
                (cols_in, meta_cols),
                (rows_in, meta_rows),
                (probs_in, box.at[:, pl.ds(0, prob_cols)]),
                (values_in, box.at[:, pl.ds(prob_cols, values_in.shape[1])]),
            ]
        )
    ]
    for copy in loads:
        copy.start()
    for copy in loads:
        copy.wait()
    groups = heads // QUERY_PER_KEY
    w = HEAD_SIZE
    tiles = out.shape[0] // TILE

    def out_copy(t):
        at = pl.ds(t * TILE, TILE)
        return pltpu.make_async_copy(placed.at[at], out.at[at], out_sem.at[t])

    key_at = iota((heads * img_most, TILE), 0)
    ats = [slice(t * TILE, (t + 1) * TILE) for t in range(tiles)]
    slot_at = iota((TILE, box_rows), 1)
    selects = [jnp.where(slot_at == meta_cols[at, 0:1], 1.0, 0.0).astype(BF16) for at in ats]
    own = [
        jnp.dot(select, box[...], preferred_element_type=F32).astype(BF16) for select in selects
    ]
    expanded = []
    for t, at in enumerate(ats):
        inside = meta_rows[1:2, at]
        expand = jnp.concatenate(
            [jnp.where(key_at == h * img_most + inside, 1.0, 0.0).astype(BF16) for h in range(heads)],
            axis=1,
        )
        expanded.append(jnp.dot(own[t][:, :prob_cols], expand, preferred_element_type=F32))
    for t, at in enumerate(ats):
        same = meta_cols[at, 1:2] == meta_rows[0:1, at]
        for g in range(groups):
            seen = jnp.concatenate(
                [
                    jnp.where(same, expanded[t][:, h * TILE : (h + 1) * TILE], 0.0).astype(BF16)
                    for h in range(g * QUERY_PER_KEY, (g + 1) * QUERY_PER_KEY)
                ],
                axis=0,
            )
            values = own[t][:, prob_cols + g * w : prob_cols + (g + 1) * w]
            attended = jnp.dot(seen, values, preferred_element_type=F32).astype(BF16)
            for i in range(QUERY_PER_KEY):
                a = (g * QUERY_PER_KEY + i) * w
                placed[at, a : a + w] = attended[i * TILE : (i + 1) * TILE]
        if t % 2 == 1:
            out_copy(t - 1).start()
            out_copy(t).start()
    for t in range(tiles):
        out_copy(t).wait()


def local(
    patches, ln_gain, ln_bias, w_proj, proj_bias, rms_gain, w_qkv, image_counts, source_shift
):
    senders = lax.axis_size("dp")
    order = shift_order(senders)
    half, d_vit = patches.shape
    rows = 2 * half
    parts = half // 64
    half_cols = w_proj.shape[1]
    qkv_cols = w_qkv.shape[1]
    groups = qkv_cols // ((QUERY_PER_KEY + 2) * HEAD_SIZE)
    heads = groups * QUERY_PER_KEY
    out_cols = heads * HEAD_SIZE
    images = source_shift.shape[0]
    img_most = TILE // (images // (rows // TILE))
    pair_slots = (images + senders - 1) // senders
    box_rows = senders * pair_slots * img_most
    prob_cols, value_cols = heads * img_most, groups * HEAD_SIZE
    chunks = box_rows // CHUNK
    hbm = pl.BlockSpec(memory_space=pl.ANY)
    dma = pltpu.SemaphoreType.DMA
    smalls = (
        ln_gain,
        ln_bias,
        proj_bias,
        rms_gain,
        image_counts.T,
        source_shift,
        jnp.asarray(rotary_table(TILE + img_most)),
    )
    probs, values, cols, lines = pl.pallas_call(
        functools.partial(kernel, senders, order),
        out_shape=[
            jax.ShapeDtypeStruct((box_rows, prob_cols), BF16),
            jax.ShapeDtypeStruct((box_rows, value_cols), BF16),
            jax.ShapeDtypeStruct((rows, LANES), I32),
            jax.ShapeDtypeStruct((8, rows), I32),
        ],
        in_specs=[hbm] * 10,
        out_specs=[hbm] * 4,
        scratch_shapes=[
            *[pltpu.VMEM(x.shape, x.dtype) for x in smalls],
            pltpu.VMEM((half, d_vit), BF16),
            pltpu.VMEM(w_proj.shape, BF16),
            pltpu.VMEM(w_qkv.shape, BF16),
            pltpu.VMEM((rows, d_vit), BF16),
            pltpu.VMEM(((rows + img_most) * (d_vit // LANES), LANES), F32),
            pltpu.VMEM((box_rows, d_vit), BF16),
            pltpu.VMEM((box_rows, 2 * half_cols), BF16),
            pltpu.VMEM((2, box_rows, LANES), F32),
            pltpu.VMEM((2, half_cols), F32),
            pltpu.VMEM((2, CHUNK, qkv_cols - value_cols), F32),
            pltpu.VMEM((box_rows, HEAD_SIZE), F32),
            pltpu.VMEM((box_rows, HEAD_SIZE), F32),
            pltpu.VMEM((box_rows, prob_cols), BF16),
            pltpu.VMEM((box_rows, value_cols), BF16),
            pltpu.VMEM((rows, LANES), I32),
            pltpu.VMEM((8, rows), I32),
            pltpu.VMEM((8, LANES), I32),
            pltpu.SMEM((8, LANES), I32),
            dma((len(smalls),)),
            dma((parts,)),
            dma((half_cols // COL_TILE,)),
            dma((2 * groups,)),
            dma,
            dma((2,)),
            dma((parts,)),
            dma((parts,)),
            dma((chunks,)),
            dma((chunks,)),
            dma((chunks,)),
            dma((chunks,)),
            dma((senders,)),
            dma((senders,)),
            dma((senders,)),
            dma((senders,)),
        ],
        compiler_params=pltpu.CompilerParams(
            collective_id=0, has_side_effects=True, vmem_limit_bytes=60 * 1024 * 1024
        ),
        name="projector_attention",
    )(
        *smalls,
        patches,
        w_proj,
        w_qkv,
    )
    return pl.pallas_call(
        functools.partial(place_kernel, heads, img_most),
        out_shape=jax.ShapeDtypeStruct((rows, out_cols), BF16),
        in_specs=[hbm] * 4,
        out_specs=hbm,
        scratch_shapes=[
            pltpu.VMEM(cols.shape, I32),
            pltpu.VMEM(lines.shape, I32),
            pltpu.VMEM((box_rows, prob_cols + value_cols), BF16),
            pltpu.VMEM((rows, out_cols), BF16),
            dma((4,)),
            dma((rows // TILE,)),
        ],
        name="place",
    )(cols, lines, probs, values)


def solution(mesh):
    in_specs = (
        P(("dp", "mp"), None),
        P(),
        P(),
        P(None, "mp"),
        P("mp"),
        P(),
        P(None, "mp"),
        P(),
        P(),
    )
    out_specs = P("dp", "mp")
    return jax.shard_map(local, mesh=mesh, in_specs=in_specs, out_specs=out_specs, check_vma=False)
```

```python
import functools

import jax
import jax.numpy as jnp
import numpy as np
from jax import lax
from jax.experimental import pallas as pl
from jax.experimental.pallas import tpu as pltpu
from jax.sharding import PartitionSpec as P

HEAD_SIZE = 128
TILE = 128
QUERY_PER_KEY = 4
COL_TILE = 512
LANES = 128
CHUNK = 256

norm_epsilon = 1e-05
rms_epsilon = 1e-05
rotary_base = 500000.0

F32 = jnp.float32
BF16 = jnp.bfloat16
I32 = jnp.int32
MESH = pl.DeviceIdType.MESH


def exclusive_or(a, b, senders):
    total, bit = 0, 1
    while bit < senders:
        total = total + lax.rem(lax.div(a, bit) + lax.div(b, bit), 2) * bit
        bit *= 2
    return total


def rotary_table(positions):
    frequency = np.float32(rotary_base) ** (
        -(np.arange(HEAD_SIZE // 2, dtype=np.float32) * np.float32(2.0 / HEAD_SIZE))
    )
    angles = np.arange(positions, dtype=np.float32)[:, None] * frequency[None, :].astype(np.float32)
    cos = np.cos(angles.astype(np.float64)).astype(np.float32)
    sin = np.sin(angles.astype(np.float64)).astype(np.float32)
    both = np.stack([np.concatenate([cos, cos], 1), np.concatenate([-sin, sin], 1)], axis=1)
    return both.reshape(2 * positions, HEAD_SIZE)


def gelu(v):
    return 0.5 * v * (1.0 + lax.erf(v * np.float32(0.5**0.5)))


def iota(shape, axis):
    return lax.broadcasted_iota(jnp.int32, shape, axis)


def lane_sum(x):
    return jnp.sum(x, axis=1, keepdims=True)


def row_sum(x):
    return jnp.sum(x, axis=0, keepdims=True)


def kernel(
    senders,
    ln_gain_in,
    ln_bias_in,
    proj_bias_in,
    rms_gain_in,
    counts_in,
    source_shift_in,
    table_in,
    patches,
    w_proj,
    w_qkv,
    box_probs,
    box_values,
    meta_cols,
    meta_rows,
    ln_gain,
    ln_bias,
    proj_bias,
    rms_gain,
    counts,
    source_shift,
    table,
    raw,
    w1,
    w2,
    normed,
    spread,
    picked,
    hidden,
    squares,
    bias,
    proj,
    cos_at,
    sin_at,
    probs_at,
    values_at,
    cols_at,
    rows_at,
    plan,
    plan_at,
    small_sem,
    raw_sem,
    w1_sem,
    w2_sem,
    plan_sem,
    meta_sem,
    norm_send,
    norm_recv,
    hid_send,
    hid_recv,
    sq_send,
    sq_recv,
    probs_sems,
    values_sems,
):
    me = lax.axis_index("dp")
    core = lax.axis_index("mp")
    peer = 1 - core
    half, d_vit = raw.shape
    rows = 2 * half
    blocks = d_vit // LANES
    box_rows = values_at.shape[0]
    block = box_rows // senders
    images = source_shift.shape[0]
    tiles_dev = rows // TILE
    img_tile = images // tiles_dev
    img_most = TILE // img_tile
    slots = box_rows // img_most
    pair_slots = block // img_most
    half_cols = w_proj.shape[1]
    qkv_cols = w_qkv.shape[1]
    groups = qkv_cols // ((QUERY_PER_KEY + 2) * HEAD_SIZE)
    tiles1 = half_cols // COL_TILE
    qk_group = (QUERY_PER_KEY + 1) * HEAD_SIZE
    qk_cols = groups * qk_group
    chunks = box_rows // CHUNK
    part = 64
    parts = half // part

    def raw_copy(i):
        at = pl.ds(i * part, part)
        return pltpu.make_async_copy(patches.at[at], raw.at[at], raw_sem.at[i])

    def w1_copy(j):
        cols = pl.ds(j * COL_TILE, COL_TILE)
        return pltpu.make_async_copy(w_proj.at[:, cols], w1.at[:, cols], w1_sem)

    def w2_copy(j):
        g = j // 2
        first = g * (qk_group + HEAD_SIZE)
        if j % 2 == 0:
            source, to, width = first, g * qk_group, qk_group
        else:
            source, to, width = first + qk_group, qk_cols + g * HEAD_SIZE, HEAD_SIZE
        return pltpu.make_async_copy(
            w_qkv.at[:, pl.ds(source, width)], w2.at[:, pl.ds(to, width)], w2_sem
        )

    smalls = [
        pltpu.make_async_copy(there, here, small_sem.at[i])
        for i, (there, here) in enumerate(
            [
                (ln_gain_in, ln_gain),
                (ln_bias_in, ln_bias),
                (counts_in, counts),
                (source_shift_in, source_shift),
                (proj_bias_in, proj_bias),
                (rms_gain_in, rms_gain),
                (table_in, table),
            ]
        )
    ]
    for copy in smalls[:2]:
        copy.start()
    for i in range(parts):
        raw_copy(i).start()
    for copy in smalls[2:]:
        copy.start()
    for j in range(tiles1 // 2):
        w1_copy(j).start()

    barrier = pltpu.get_barrier_semaphore()
    pl.semaphore_signal(barrier, inc=1, device_id={"mp": peer}, device_id_type=MESH)
    for v in range(1, senders):
        pl.semaphore_signal(
            barrier, inc=1, device_id={"dp": lax.rem(me + v, senders)}, device_id_type=MESH
        )

    for copy in smalls[:2]:
        copy.wait()
    for j in range(tiles1 // 2, tiles1):
        w1_copy(j).start()
    gain_f = ln_gain[...].reshape(1, -1).astype(F32)
    bias_f = ln_bias[...].reshape(1, -1).astype(F32)
    def widen(first, values):
        for h in range(2):
            for b in range(blocks):
                at = pl.ds((first + 8 * h) * blocks + b, 8, stride=blocks)
                spread[at, :] = values[8 * h : 8 * h + 8, b * LANES : (b + 1) * LANES]

    def norm_copy(i):
        mine = normed.at[pl.ds(pl.multiple_of(core * half + i * part, part), part)]
        return pltpu.make_async_remote_copy(
            src_ref=mine,
            dst_ref=mine,
            send_sem=norm_send,
            recv_sem=norm_recv.at[i],
            device_id={"mp": peer},
            device_id_type=MESH,
        )

    for i in range(parts):
        raw_copy(i).wait()

        @pl.loop(0, part // 16, unroll=4)
        def _(r):
            values = raw[pl.ds(pl.multiple_of(i * part + r * 16, 16), 16), :].astype(F32)
            centred = values - jnp.mean(values, axis=-1, keepdims=True)
            variance = jnp.mean(centred * centred, axis=-1, keepdims=True)
            scaled = centred * lax.rsqrt(variance + norm_epsilon) * gain_f + bias_f
            first = pl.multiple_of(core * half + i * part + r * 16, 16)
            normed[pl.ds(first, 16), :] = scaled.astype(BF16)
            widen(first, scaled)

        if i == 0:
            pl.semaphore_wait(barrier, senders)
        norm_copy(i).start()

    for copy in smalls[2:]:
        copy.wait()
    sq = (images, images)
    k_at, l_at = iota(sq, 0), iota(sq, 1)
    eye = k_at == l_at
    before = l_at < k_at

    def to_row(col):
        return row_sum(jnp.where(eye, col, 0))

    def to_col(row):
        return lane_sum(jnp.where(eye, row, 0))

    tiles_all = counts.shape[1]
    image_counts = counts[...]
    earlier = jnp.zeros((img_tile, tiles_all), I32)
    for j in range(img_tile - 1):
        earlier += jnp.where(iota((img_tile, tiles_all), 0) > j, image_counts[j : j + 1, :], 0)
    counts_by = jnp.concatenate([image_counts] * tiles_dev, axis=0)
    earlier_by = jnp.concatenate([earlier] * tiles_dev, axis=0)
    tile_at = iota((images, tiles_all), 1)
    own_tile = iota((images, 1), 0) // img_tile

    shift_row = source_shift[...].reshape(1, images)
    shift = to_col(shift_row)
    dest = me - shift
    dest = jnp.where(dest < 0, dest + senders, dest)
    source = lax.rem(me + shift, senders)
    there = tile_at == dest * tiles_dev + own_tile
    starts = lane_sum(jnp.where(before, to_row(lane_sum(jnp.where(there, counts_by, 0))), 0))
    far_offset = lane_sum(jnp.where(there, earlier_by, 0))
    rank = lane_sum(jnp.where(before & (shift_row == shift), 1, 0))

    def slot_of(partner):
        apart = exclusive_or(jnp.broadcast_to(me, partner.shape), partner, senders)
        return (senders - 1 - apart) * pair_slots + rank

    slot = slot_of(dest)

    slot_hit = slot == iota((images, LANES), 1)
    plan[0:1, :] = row_sum(jnp.where(slot_hit, starts * blocks, 0))
    plan[1:2, :] = row_sum(jnp.where(slot_hit, far_offset * 2, 0))
    plan_copy = pltpu.make_async_copy(plan, plan_at, plan_sem)
    plan_copy.start()

    bias[0:1, :] = proj_bias[...].reshape(1, -1).astype(F32)
    gains = rms_gain[...].reshape(1, -1).astype(F32)
    bias[1:2, :] = jnp.where(core == 0, gains[:, :half_cols], gains[:, half_cols:])

    spread[rows * blocks :, :] = jnp.zeros((img_most * blocks, LANES), F32)

    here = tile_at == me * tiles_dev + own_tile
    my_col = lane_sum(jnp.where(here, counts_by, 0))
    my_off = lane_sum(jnp.where(here, earlier_by, 0))
    my_row = to_row(my_col)
    my_off_row = to_row(my_off)
    slot_row = to_row(slot_of(source))
    image_row, t_col = iota((TILE, images), 1), iota((TILE, images), 0)
    image_col, t_row = iota((images, TILE), 0), iota((images, TILE), 1)
    lane_at = iota((TILE, LANES), 1)
    for t in range(tiles_dev):
        hit = (image_row // img_tile == t) & (t_col >= my_off_row) & (t_col < my_off_row + my_row)
        box_at = lane_sum(jnp.where(hit, slot_row * img_most + (t_col - my_off_row) + 1, 0)) - 1
        off_at = lane_sum(jnp.where(hit, my_off_row + 1, 0)) - 1
        cols_at[t * TILE : (t + 1) * TILE, :] = jnp.where(lane_at == 0, box_at, off_at)
        hit = (image_col // img_tile == t) & (t_row >= my_off) & (t_row < my_off + my_col)
        rows_at[0:1, t * TILE : (t + 1) * TILE] = row_sum(jnp.where(hit, my_off + 1, 0)) - 1
        rows_at[1:2, t * TILE : (t + 1) * TILE] = row_sum(jnp.where(hit, t_row - my_off + 1, 0)) - 1
    meta = [
        pltpu.make_async_copy(cols_at, meta_cols, meta_sem.at[0]),
        pltpu.make_async_copy(rows_at, meta_rows, meta_sem.at[1]),
    ]
    for copy in meta:
        copy.start()

    plan_copy.wait()

    @pl.loop(0, slots, unroll=4)
    def _(i):
        first = plan_at[1, i]
        for h in range(img_most // 8):
            to = pl.ds(pl.multiple_of(i * img_most + 8 * h, 8), 8)
            cos_at[to, :] = table[pl.ds(first + 16 * h, 8, stride=2), :]
            sin_at[to, :] = table[pl.ds(first + 16 * h + 1, 8, stride=2), :]

    for i in range(parts):
        norm_copy(i).wait_recv()

        @pl.loop(0, part // 16, unroll=2)
        def _(r):
            first = pl.multiple_of(peer * half + i * part + r * 16, 16)
            widen(first, normed[pl.ds(first, 16), :].astype(F32))

    mine = pl.ds(pl.multiple_of(core * half_cols, half_cols), half_cols)

    def to_peer(ref, send_sem, recv_sem):
        return pltpu.make_async_remote_copy(
            src_ref=ref,
            dst_ref=ref,
            send_sem=send_sem,
            recv_sem=recv_sem,
            device_id={"mp": peer},
            device_id_type=MESH,
        )

    def copy_hidden(c):
        return to_peer(hidden.at[pl.ds(c * CHUNK, CHUNK), mine], hid_send.at[c], hid_recv.at[c])

    def copy_squares(c):
        return to_peer(squares.at[core, pl.ds(c * CHUNK, CHUNK)], sq_send.at[c], sq_recv.at[c])

    far_rows = pl.ds(0, box_rows - block)

    def exchange(o, outbox, inbox, sems):
        at = pl.ds(o * block, block)
        if o == senders - 1:
            return pltpu.make_async_copy(outbox.at[at], inbox.at[at], sems.at[2])
        return pltpu.make_async_remote_copy(
            src_ref=outbox.at[at],
            dst_ref=inbox.at[at],
            send_sem=sems.at[0],
            recv_sem=sems.at[1],
            device_id={"dp": exclusive_or(me, senders - 1 - o, senders)},
            device_id_type=MESH,
        )

    def copy_probs(o):
        return exchange(o, probs_at, box_probs, probs_sems)

    def copy_values(o):
        return exchange(o, values_at, box_values, values_sems)

    slots_chunk = CHUNK // img_most

    def pick(i):
        first = plan_at[0, i]
        to = pl.ds(pl.multiple_of(i * img_most, img_most), img_most)
        for b in range(blocks):
            picked[to, b * LANES : (b + 1) * LANES] = jnp.concatenate(
                [
                    spread[pl.ds(first + 8 * h * blocks + b, 8, stride=blocks), :]
                    for h in range(img_most // 8)
                ],
                axis=0,
            ).astype(BF16)

    def project(c, low, high):
        at = pl.ds(c * CHUNK, CHUNK)
        for j in range(low, high):
            cols = slice(j * COL_TILE, (j + 1) * COL_TILE)
            pre = jnp.dot(picked[at, :], w1[:, cols], preferred_element_type=F32)
            if c == 0 and chunks > 1:
                for i in range(slots_chunk * j // tiles1, slots_chunk * (j + 1) // tiles1):
                    pick(slots_chunk + i)
            y = gelu(pre + bias[0:1, cols])
            z = y * y
            total = z[:, :LANES]
            for b in range(1, COL_TILE // LANES):
                total = total + z[:, b * LANES : (b + 1) * LANES]
            if j == 0:
                squares[core, at, :] = total
            else:
                squares[core, at, :] += total
            to = pl.ds(pl.multiple_of(core * half_cols + j * COL_TILE, COL_TILE), COL_TILE)
            hidden[at, to] = (y * bias[1:2, cols]).astype(BF16)

    def send(c):
        copy_squares(c).start()
        copy_hidden(c).start()

    wide_at = iota((img_most, QUERY_PER_KEY * TILE), 1)
    causal = iota((img_most, QUERY_PER_KEY * TILE), 0) <= wide_at % img_most
    own_image = (wide_at % TILE) // img_most
    w = HEAD_SIZE

    def product(c, cols):
        return jnp.dot(hidden[pl.ds(c * CHUNK, CHUNK), :], w2[:, cols], preferred_element_type=F32)

    qk_tiles = [slice(f, min(f + COL_TILE, qk_cols)) for f in range(0, qk_cols, COL_TILE)]

    def qk(c, j):
        proj[c % 2, :, qk_tiles[j]] = product(c, qk_tiles[j])

    def arrived(c):
        copy_squares(c).wait_recv()
        copy_hidden(c).wait_recv()

    def values(c, work):
        at = pl.ds(c * CHUNK, CHUNK)
        total = lane_sum(squares[0, at, :] + squares[1, at, :])
        scale = lax.rsqrt(total * (1.0 / (2 * half_cols)) + rms_epsilon)
        value_rows = product(c, slice(qk_cols, qkv_cols))
        work()
        values_at[at, :] = (value_rows * scale).astype(BF16)
        cos_at[at, :] *= scale
        sin_at[at, :] *= scale

    def send_values(c):
        for o in range(c * CHUNK // block, (c + 1) * CHUNK // block):
            copy_values(o).start()

    def attend(c, first):
        to = pl.ds(c * CHUNK + first, TILE)
        cos = cos_at[to, :]
        sin = sin_at[to, :]

        def turned(h):
            v = proj[c % 2, first : first + TILE, h * w : (h + 1) * w]
            return (v * cos + pltpu.roll(v, w // 2, 1) * sin).astype(BF16)

        seen = []
        for g in range(groups):
            h0 = g * (QUERY_PER_KEY + 1)
            q = jnp.concatenate([turned(h0 + i) for i in range(QUERY_PER_KEY)], axis=0)
            k = turned(h0 + QUERY_PER_KEY)
            scores = lax.dot_general(
                k, q, (((1,), (1,)), ((), ())), preferred_element_type=F32
            )
            kept = scores[:img_most]
            for j in range(1, img_tile):
                kept = jnp.where(own_image == j, scores[j * img_most : (j + 1) * img_most], kept)
            kept = jnp.where(causal, kept * np.float32(HEAD_SIZE ** (-0.5)), -1e30)
            weights = jnp.exp(kept - jnp.max(kept, axis=0, keepdims=True))
            probs = weights / row_sum(weights)
            seen += [probs[:, i * TILE : (i + 1) * TILE] for i in range(QUERY_PER_KEY)]
        probs_at[to, :] = jnp.concatenate(seen, axis=0).T.astype(BF16)

    def send_probs(c, first):
        for o in range((c * CHUNK + first) // block, (c * CHUNK + first + TILE) // block):
            copy_probs(o).start()


    pl.loop(0, slots_chunk, unroll=2)(pick)
    if chunks > 2:
        pl.loop(2 * slots_chunk, slots, unroll=2)(pick)
    pltpu.make_async_copy(w_proj, w1, w1_sem).wait()
    for j in range(2 * groups):
        w2_copy(j).start()
    project(0, 0, tiles1)
    send(0)
    tiles = CHUNK // TILE
    for c in range(chunks):
        more = c + 1 < chunks
        if c == 0:
            if more:
                project(1, 0, tiles1 - 1)
            arrived(0)
            pltpu.make_async_copy(w_qkv, w2, w2_sem).wait()
            values(0, lambda: project(1, tiles1 - 1, tiles1) if more else None)
            send_values(0)
            if more:
                send(1)
            for j in range(len(qk_tiles)):
                qk(0, j)
        if c + 2 < chunks:
            project(c + 2, 0, tiles1)
        if more:
            arrived(c + 1)
            if c + 2 < chunks:
                send(c + 2)

            def beside():
                qk(c + 1, 0)
                for t in range(tiles):
                    attend(c, t * TILE)

            values(c + 1, beside)
            for t in range(tiles):
                send_probs(c, t * TILE)
            send_values(c + 1)
            for j in range(1, len(qk_tiles)):
                qk(c + 1, j)
        else:
            for t in range(tiles):
                attend(c, t * TILE)
                send_probs(c, t * TILE)

    for outbox, inbox, sems in (
        (values_at, box_values, values_sems),
        (probs_at, box_probs, probs_sems),
    ):
        exchange(senders - 1, outbox, inbox, sems).wait()
        landed = inbox.at[far_rows]
        pltpu.make_async_copy(landed, landed, sems.at[1]).wait()
    for copy in meta:
        copy.wait()
    sent = normed.at[pl.ds(pl.multiple_of(core * half, half), half)]
    pltpu.make_async_copy(sent, sent, norm_send).wait()
    for c in range(chunks):
        copy_squares(c).wait_send()
        copy_hidden(c).wait_send()
    for outbox, sems in ((values_at, values_sems), (probs_at, probs_sems)):
        left = outbox.at[far_rows]
        pltpu.make_async_copy(left, left, sems.at[0]).wait()


def place_kernel(heads, img_most, *refs):
    cols_in, rows_in, probs_in, values_in, out, meta_cols, meta_rows, box, placed, in_sem, out_sem = refs
    box_rows, prob_cols = probs_in.shape
    loads = [
        pltpu.make_async_copy(there, here, in_sem.at[i])
        for i, (there, here) in enumerate(
            [
                (cols_in, meta_cols),
                (rows_in, meta_rows),
                (probs_in, box.at[:, pl.ds(0, prob_cols)]),
                (values_in, box.at[:, pl.ds(prob_cols, values_in.shape[1])]),
            ]
        )
    ]
    for copy in loads:
        copy.start()
    for copy in loads:
        copy.wait()
    groups = heads // QUERY_PER_KEY
    w = HEAD_SIZE
    tiles = out.shape[0] // TILE

    def out_copy(t):
        at = pl.ds(t * TILE, TILE)
        return pltpu.make_async_copy(placed.at[at], out.at[at], out_sem.at[t])

    key_at = iota((heads * img_most, TILE), 0)
    ats = [slice(t * TILE, (t + 1) * TILE) for t in range(tiles)]
    slot_at = iota((TILE, box_rows), 1)
    selects = [jnp.where(slot_at == meta_cols[at, 0:1], 1.0, 0.0).astype(BF16) for at in ats]
    own = [
        jnp.dot(select, box[...], preferred_element_type=F32).astype(BF16) for select in selects
    ]
    expanded = []
    for t, at in enumerate(ats):
        inside = meta_rows[1:2, at]
        expand = jnp.concatenate(
            [jnp.where(key_at == h * img_most + inside, 1.0, 0.0).astype(BF16) for h in range(heads)],
            axis=1,
        )
        expanded.append(jnp.dot(own[t][:, :prob_cols], expand, preferred_element_type=F32))
    for t, at in enumerate(ats):
        same = meta_cols[at, 1:2] == meta_rows[0:1, at]
        for g in range(groups):
            seen = jnp.concatenate(
                [
                    jnp.where(same, expanded[t][:, h * TILE : (h + 1) * TILE], 0.0).astype(BF16)
                    for h in range(g * QUERY_PER_KEY, (g + 1) * QUERY_PER_KEY)
                ],
                axis=0,
            )
            values = own[t][:, prob_cols + g * w : prob_cols + (g + 1) * w]
            attended = jnp.dot(seen, values, preferred_element_type=F32).astype(BF16)
            for i in range(QUERY_PER_KEY):
                a = (g * QUERY_PER_KEY + i) * w
                placed[at, a : a + w] = attended[i * TILE : (i + 1) * TILE]
        if t % 2 == 1:
            out_copy(t - 1).start()
            out_copy(t).start()
    for t in range(tiles):
        out_copy(t).wait()


def local(
    patches, ln_gain, ln_bias, w_proj, proj_bias, rms_gain, w_qkv, image_counts, source_shift
):
    senders = lax.axis_size("dp")
    half, d_vit = patches.shape
    rows = 2 * half
    parts = half // 64
    half_cols = w_proj.shape[1]
    qkv_cols = w_qkv.shape[1]
    groups = qkv_cols // ((QUERY_PER_KEY + 2) * HEAD_SIZE)
    heads = groups * QUERY_PER_KEY
    out_cols = heads * HEAD_SIZE
    images = source_shift.shape[0]
    img_most = TILE // (images // (rows // TILE))
    pair_slots = (images + senders - 1) // senders
    box_rows = senders * pair_slots * img_most
    prob_cols, value_cols = heads * img_most, groups * HEAD_SIZE
    chunks = box_rows // CHUNK
    hbm = pl.BlockSpec(memory_space=pl.ANY)
    dma = pltpu.SemaphoreType.DMA
    smalls = (
        ln_gain,
        ln_bias,
        proj_bias,
        rms_gain,
        image_counts.T,
        source_shift,
        jnp.asarray(rotary_table(TILE + img_most)),
    )
    probs, values, cols, lines = pl.pallas_call(
        functools.partial(kernel, senders),
        out_shape=[
            jax.ShapeDtypeStruct((box_rows, prob_cols), BF16),
            jax.ShapeDtypeStruct((box_rows, value_cols), BF16),
            jax.ShapeDtypeStruct((rows, LANES), I32),
            jax.ShapeDtypeStruct((8, rows), I32),
        ],
        in_specs=[hbm] * 10,
        out_specs=[hbm] * 4,
        scratch_shapes=[
            *[pltpu.VMEM(x.shape, x.dtype) for x in smalls],
            pltpu.VMEM((half, d_vit), BF16),
            pltpu.VMEM(w_proj.shape, BF16),
            pltpu.VMEM(w_qkv.shape, BF16),
            pltpu.VMEM((rows, d_vit), BF16),
            pltpu.VMEM(((rows + img_most) * (d_vit // LANES), LANES), F32),
            pltpu.VMEM((box_rows, d_vit), BF16),
            pltpu.VMEM((box_rows, 2 * half_cols), BF16),
            pltpu.VMEM((2, box_rows, LANES), F32),
            pltpu.VMEM((2, half_cols), F32),
            pltpu.VMEM((2, CHUNK, qkv_cols - value_cols), F32),
            pltpu.VMEM((box_rows, HEAD_SIZE), F32),
            pltpu.VMEM((box_rows, HEAD_SIZE), F32),
            pltpu.VMEM((box_rows, prob_cols), BF16),
            pltpu.VMEM((box_rows, value_cols), BF16),
            pltpu.VMEM((rows, LANES), I32),
            pltpu.VMEM((8, rows), I32),
            pltpu.VMEM((8, LANES), I32),
            pltpu.SMEM((8, LANES), I32),
            dma((len(smalls),)),
            dma((parts,)),
            dma,
            dma,
            dma,
            dma((2,)),
            dma,
            dma((parts,)),
            dma((chunks,)),
            dma((chunks,)),
            dma((chunks,)),
            dma((chunks,)),
            dma((3,)),
            dma((3,)),
        ],
        compiler_params=pltpu.CompilerParams(
            collective_id=0, has_side_effects=True, vmem_limit_bytes=60 * 1024 * 1024
        ),
        name="projector_attention",
    )(
        *smalls,
        patches,
        w_proj,
        w_qkv,
    )
    return pl.pallas_call(
        functools.partial(place_kernel, heads, img_most),
        out_shape=jax.ShapeDtypeStruct((rows, out_cols), BF16),
        in_specs=[hbm] * 4,
        out_specs=hbm,
        scratch_shapes=[
            pltpu.VMEM(cols.shape, I32),
            pltpu.VMEM(lines.shape, I32),
            pltpu.VMEM((box_rows, prob_cols + value_cols), BF16),
            pltpu.VMEM((rows, out_cols), BF16),
            dma((4,)),
            dma((rows // TILE,)),
        ],
        name="place",
    )(cols, lines, probs, values)


def solution(mesh):
    in_specs = (
        P(("dp", "mp"), None),
        P(),
        P(),
        P(None, "mp"),
        P("mp"),
        P(),
        P(None, "mp"),
        P(),
        P(),
    )
    out_specs = P("dp", "mp")
    return jax.shard_map(local, mesh=mesh, in_specs=in_specs, out_specs=out_specs, check_vma=False)
```

```python
import functools

import jax
import jax.numpy as jnp
import numpy as np
from jax import lax
from jax.experimental import pallas as pl
from jax.experimental.pallas import tpu as pltpu
from jax.sharding import PartitionSpec as P

HEAD_SIZE = 128
TILE = 128
QUERY_PER_KEY = 4
COL_TILE = 512
LANES = 128
CHUNK = 256

norm_epsilon = 1e-05
rms_epsilon = 1e-05
rotary_base = 500000.0

F32 = jnp.float32
BF16 = jnp.bfloat16
I32 = jnp.int32
MESH = pl.DeviceIdType.MESH


def exclusive_or(a, b, senders):
    total, bit = 0, 1
    while bit < senders:
        total = total + lax.rem(lax.div(a, bit) + lax.div(b, bit), 2) * bit
        bit *= 2
    return total


def rotary_table(positions):
    frequency = np.float32(rotary_base) ** (
        -(np.arange(HEAD_SIZE // 2, dtype=np.float32) * np.float32(2.0 / HEAD_SIZE))
    )
    angles = np.arange(positions, dtype=np.float32)[:, None] * frequency[None, :].astype(np.float32)
    cos = np.cos(angles.astype(np.float64)).astype(np.float32)
    sin = np.sin(angles.astype(np.float64)).astype(np.float32)
    both = np.stack([np.concatenate([cos, cos], 1), np.concatenate([-sin, sin], 1)], axis=1)
    return both.reshape(2 * positions, HEAD_SIZE)


def gelu(v):
    return 0.5 * v * (1.0 + lax.erf(v * np.float32(0.5**0.5)))


def iota(shape, axis):
    return lax.broadcasted_iota(jnp.int32, shape, axis)


def lane_sum(x):
    return jnp.sum(x, axis=1, keepdims=True)


def row_sum(x):
    return jnp.sum(x, axis=0, keepdims=True)


def kernel(
    senders,
    ln_gain_in,
    ln_bias_in,
    proj_bias_in,
    rms_gain_in,
    counts_in,
    source_shift_in,
    table_in,
    patches,
    w_proj,
    w_qkv,
    box_probs,
    box_values,
    meta_cols,
    meta_rows,
    ln_gain,
    ln_bias,
    proj_bias,
    rms_gain,
    counts,
    source_shift,
    table,
    raw,
    w1,
    w2,
    normed,
    spread,
    picked,
    hidden,
    squares,
    bias,
    proj,
    cos_at,
    sin_at,
    probs_at,
    values_at,
    cols_at,
    rows_at,
    plan,
    plan_at,
    small_sem,
    raw_sem,
    w1_sem,
    w2_sem,
    plan_sem,
    meta_sem,
    norm_send,
    norm_recv,
    hid_send,
    hid_recv,
    sq_send,
    sq_recv,
    probs_sems,
    values_sems,
):
    me = lax.axis_index("dp")
    core = lax.axis_index("mp")
    peer = 1 - core
    half, d_vit = raw.shape
    rows = 2 * half
    blocks = d_vit // LANES
    box_rows = values_at.shape[0]
    block = box_rows // senders
    images = source_shift.shape[0]
    tiles_dev = rows // TILE
    img_tile = images // tiles_dev
    img_most = TILE // img_tile
    slots = box_rows // img_most
    pair_slots = block // img_most
    half_cols = w_proj.shape[1]
    qkv_cols = w_qkv.shape[1]
    groups = qkv_cols // ((QUERY_PER_KEY + 2) * HEAD_SIZE)
    tiles1 = half_cols // COL_TILE
    qk_group = (QUERY_PER_KEY + 1) * HEAD_SIZE
    qk_cols = groups * qk_group
    chunks = box_rows // CHUNK
    part = 64
    parts = half // part

    def raw_copy(i):
        at = pl.ds(i * part, part)
        return pltpu.make_async_copy(patches.at[at], raw.at[at], raw_sem.at[i])

    def w1_copy(j):
        cols = pl.ds(j * COL_TILE, COL_TILE)
        return pltpu.make_async_copy(w_proj.at[:, cols], w1.at[:, cols], w1_sem)

    def w2_copy(j):
        g = j // 2
        first = g * (qk_group + HEAD_SIZE)
        if j % 2 == 0:
            source, to, width = first, g * qk_group, qk_group
        else:
            source, to, width = first + qk_group, qk_cols + g * HEAD_SIZE, HEAD_SIZE
        return pltpu.make_async_copy(
            w_qkv.at[:, pl.ds(source, width)], w2.at[:, pl.ds(to, width)], w2_sem
        )

    smalls = [
        pltpu.make_async_copy(there, here, small_sem.at[i])
        for i, (there, here) in enumerate(
            [
                (ln_gain_in, ln_gain),
                (ln_bias_in, ln_bias),
                (counts_in, counts),
                (source_shift_in, source_shift),
                (proj_bias_in, proj_bias),
                (rms_gain_in, rms_gain),
                (table_in, table),
            ]
        )
    ]
    barrier = pltpu.get_barrier_semaphore()
    pl.semaphore_signal(barrier, inc=1, device_id={"mp": peer}, device_id_type=MESH)
    for v in range(1, senders):
        pl.semaphore_signal(
            barrier, inc=1, device_id={"dp": lax.rem(me + v, senders)}, device_id_type=MESH
        )

    for copy in smalls[:2]:
        copy.start()
    for i in range(parts):
        raw_copy(i).start()
    for copy in smalls[2:]:
        copy.start()
    for j in range(tiles1 // 2):
        w1_copy(j).start()

    for copy in smalls[:2]:
        copy.wait()
    for j in range(tiles1 // 2, tiles1):
        w1_copy(j).start()
    gain_f = ln_gain[...].reshape(1, -1).astype(F32)
    bias_f = ln_bias[...].reshape(1, -1).astype(F32)
    def widen(first, values):
        for h in range(2):
            for b in range(blocks):
                at = pl.ds((first + 8 * h) * blocks + b, 8, stride=blocks)
                spread[at, :] = values[8 * h : 8 * h + 8, b * LANES : (b + 1) * LANES]

    def norm_copy(i):
        mine = normed.at[pl.ds(pl.multiple_of(core * half + i * part, part), part)]
        return pltpu.make_async_remote_copy(
            src_ref=mine,
            dst_ref=mine,
            send_sem=norm_send,
            recv_sem=norm_recv.at[i],
            device_id={"mp": peer},
            device_id_type=MESH,
        )

    for i in range(parts):
        raw_copy(i).wait()

        @pl.loop(0, part // 16, unroll=4)
        def _(r):
            values = raw[pl.ds(pl.multiple_of(i * part + r * 16, 16), 16), :].astype(F32)
            centred = values - jnp.mean(values, axis=-1, keepdims=True)
            variance = jnp.mean(centred * centred, axis=-1, keepdims=True)
            scaled = centred * lax.rsqrt(variance + norm_epsilon) * gain_f + bias_f
            first = pl.multiple_of(core * half + i * part + r * 16, 16)
            normed[pl.ds(first, 16), :] = scaled.astype(BF16)
            widen(first, scaled)

        if i == 0:
            pl.semaphore_wait(barrier, senders)
        norm_copy(i).start()

    for copy in smalls[2:]:
        copy.wait()
    sq = (images, images)
    k_at, l_at = iota(sq, 0), iota(sq, 1)
    eye = k_at == l_at
    before = l_at < k_at

    def to_row(col):
        return row_sum(jnp.where(eye, col, 0))

    def to_col(row):
        return lane_sum(jnp.where(eye, row, 0))

    tiles_all = counts.shape[1]
    image_counts = counts[...]
    earlier = jnp.zeros((img_tile, tiles_all), I32)
    for j in range(img_tile - 1):
        earlier += jnp.where(iota((img_tile, tiles_all), 0) > j, image_counts[j : j + 1, :], 0)
    counts_by = jnp.concatenate([image_counts] * tiles_dev, axis=0)
    earlier_by = jnp.concatenate([earlier] * tiles_dev, axis=0)
    tile_at = iota((images, tiles_all), 1)
    own_tile = iota((images, 1), 0) // img_tile

    shift_row = source_shift[...].reshape(1, images)
    shift = to_col(shift_row)
    dest = me - shift
    dest = jnp.where(dest < 0, dest + senders, dest)
    source = lax.rem(me + shift, senders)
    there = tile_at == dest * tiles_dev + own_tile
    starts = lane_sum(jnp.where(before, to_row(lane_sum(jnp.where(there, counts_by, 0))), 0))
    far_offset = lane_sum(jnp.where(there, earlier_by, 0))
    rank = lane_sum(jnp.where(before & (shift_row == shift), 1, 0))

    def slot_of(partner):
        apart = exclusive_or(jnp.broadcast_to(me, partner.shape), partner, senders)
        return (senders - 1 - apart) * pair_slots + rank

    slot = slot_of(dest)

    slot_hit = slot == iota((images, LANES), 1)
    plan[0:1, :] = row_sum(jnp.where(slot_hit, starts * blocks, 0))
    plan[1:2, :] = row_sum(jnp.where(slot_hit, far_offset * 2, 0))
    plan_copy = pltpu.make_async_copy(plan, plan_at, plan_sem)
    plan_copy.start()

    bias[0:1, :] = proj_bias[...].reshape(1, -1).astype(F32)
    gains = rms_gain[...].reshape(1, -1).astype(F32)
    bias[1:2, :] = jnp.where(core == 0, gains[:, :half_cols], gains[:, half_cols:])

    spread[rows * blocks :, :] = jnp.zeros((img_most * blocks, LANES), F32)

    here = tile_at == me * tiles_dev + own_tile
    my_col = lane_sum(jnp.where(here, counts_by, 0))
    my_off = lane_sum(jnp.where(here, earlier_by, 0))
    my_row = to_row(my_col)
    my_off_row = to_row(my_off)
    slot_row = to_row(slot_of(source))
    image_row, t_col = iota((TILE, images), 1), iota((TILE, images), 0)
    image_col, t_row = iota((images, TILE), 0), iota((images, TILE), 1)
    lane_at = iota((TILE, LANES), 1)
    for t in range(tiles_dev):
        hit = (image_row // img_tile == t) & (t_col >= my_off_row) & (t_col < my_off_row + my_row)
        box_at = lane_sum(jnp.where(hit, slot_row * img_most + (t_col - my_off_row) + 1, 0)) - 1
        off_at = lane_sum(jnp.where(hit, my_off_row + 1, 0)) - 1
        cols_at[t * TILE : (t + 1) * TILE, :] = jnp.where(lane_at == 0, box_at, off_at)
        hit = (image_col // img_tile == t) & (t_row >= my_off) & (t_row < my_off + my_col)
        rows_at[0:1, t * TILE : (t + 1) * TILE] = row_sum(jnp.where(hit, my_off + 1, 0)) - 1
        rows_at[1:2, t * TILE : (t + 1) * TILE] = row_sum(jnp.where(hit, t_row - my_off + 1, 0)) - 1
    meta = [
        pltpu.make_async_copy(cols_at, meta_cols, meta_sem.at[0]),
        pltpu.make_async_copy(rows_at, meta_rows, meta_sem.at[1]),
    ]
    for copy in meta:
        copy.start()

    plan_copy.wait()

    @pl.loop(0, slots, unroll=4)
    def _(i):
        first = plan_at[1, i]
        for h in range(img_most // 8):
            to = pl.ds(pl.multiple_of(i * img_most + 8 * h, 8), 8)
            cos_at[to, :] = table[pl.ds(first + 16 * h, 8, stride=2), :]
            sin_at[to, :] = table[pl.ds(first + 16 * h + 1, 8, stride=2), :]

    for i in range(parts):
        norm_copy(i).wait_recv()

        @pl.loop(0, part // 16, unroll=2)
        def _(r):
            first = pl.multiple_of(peer * half + i * part + r * 16, 16)
            widen(first, normed[pl.ds(first, 16), :].astype(F32))

    mine = pl.ds(pl.multiple_of(core * half_cols, half_cols), half_cols)

    def to_peer(ref, send_sem, recv_sem):
        return pltpu.make_async_remote_copy(
            src_ref=ref,
            dst_ref=ref,
            send_sem=send_sem,
            recv_sem=recv_sem,
            device_id={"mp": peer},
            device_id_type=MESH,
        )

    def copy_hidden(c):
        return to_peer(hidden.at[pl.ds(c * CHUNK, CHUNK), mine], hid_send.at[c], hid_recv.at[c])

    def copy_squares(c):
        return to_peer(squares.at[core, pl.ds(c * CHUNK, CHUNK)], sq_send.at[c], sq_recv.at[c])

    far_rows = pl.ds(0, box_rows - block)

    def exchange(o, outbox, inbox, sems):
        at = pl.ds(o * block, block)
        if o == senders - 1:
            return pltpu.make_async_copy(outbox.at[at], inbox.at[at], sems.at[2])
        return pltpu.make_async_remote_copy(
            src_ref=outbox.at[at],
            dst_ref=inbox.at[at],
            send_sem=sems.at[0],
            recv_sem=sems.at[1],
            device_id={"dp": exclusive_or(me, senders - 1 - o, senders)},
            device_id_type=MESH,
        )

    def copy_probs(o):
        return exchange(o, probs_at, box_probs, probs_sems)

    def copy_values(o):
        return exchange(o, values_at, box_values, values_sems)

    slots_chunk = CHUNK // img_most

    def pick(i):
        first = plan_at[0, i]
        to = pl.ds(pl.multiple_of(i * img_most, img_most), img_most)
        for b in range(blocks):
            picked[to, b * LANES : (b + 1) * LANES] = jnp.concatenate(
                [
                    spread[pl.ds(first + 8 * h * blocks + b, 8, stride=blocks), :]
                    for h in range(img_most // 8)
                ],
                axis=0,
            ).astype(BF16)

    def project(c, low, high):
        at = pl.ds(c * CHUNK, CHUNK)
        for j in range(low, high):
            cols = slice(j * COL_TILE, (j + 1) * COL_TILE)
            pre = jnp.dot(picked[at, :], w1[:, cols], preferred_element_type=F32)
            if c == 0 and chunks > 1:
                for i in range(slots_chunk * j // tiles1, slots_chunk * (j + 1) // tiles1):
                    pick(slots_chunk + i)
            y = gelu(pre + bias[0:1, cols])
            z = y * y
            total = z[:, :LANES]
            for b in range(1, COL_TILE // LANES):
                total = total + z[:, b * LANES : (b + 1) * LANES]
            if j == 0:
                squares[core, at, :] = total
            else:
                squares[core, at, :] += total
            to = pl.ds(pl.multiple_of(core * half_cols + j * COL_TILE, COL_TILE), COL_TILE)
            hidden[at, to] = (y * bias[1:2, cols]).astype(BF16)

    def send(c):
        copy_squares(c).start()
        copy_hidden(c).start()

    wide_at = iota((img_most, QUERY_PER_KEY * TILE), 1)
    causal = iota((img_most, QUERY_PER_KEY * TILE), 0) <= wide_at % img_most
    own_image = (wide_at % TILE) // img_most
    w = HEAD_SIZE

    def product(c, cols):
        return jnp.dot(hidden[pl.ds(c * CHUNK, CHUNK), :], w2[:, cols], preferred_element_type=F32)

    qk_tiles = [slice(f, min(f + COL_TILE, qk_cols)) for f in range(0, qk_cols, COL_TILE)]

    def qk(c, j):
        proj[c % 2, :, qk_tiles[j]] = product(c, qk_tiles[j])

    def arrived(c):
        copy_squares(c).wait_recv()
        copy_hidden(c).wait_recv()

    def values(c, work):
        at = pl.ds(c * CHUNK, CHUNK)
        total = lane_sum(squares[0, at, :] + squares[1, at, :])
        scale = lax.rsqrt(total * (1.0 / (2 * half_cols)) + rms_epsilon)
        value_rows = product(c, slice(qk_cols, qkv_cols))
        work()
        values_at[at, :] = (value_rows * scale).astype(BF16)
        cos_at[at, :] *= scale
        sin_at[at, :] *= scale

    def send_values(c):
        for o in range(c * CHUNK // block, (c + 1) * CHUNK // block):
            copy_values(o).start()

    def attend(c, first):
        to = pl.ds(c * CHUNK + first, TILE)
        cos = cos_at[to, :]
        sin = sin_at[to, :]

        def turned(h):
            v = proj[c % 2, first : first + TILE, h * w : (h + 1) * w]
            return (v * cos + pltpu.roll(v, w // 2, 1) * sin).astype(BF16)

        seen = []
        for g in range(groups):
            h0 = g * (QUERY_PER_KEY + 1)
            q = jnp.concatenate([turned(h0 + i) for i in range(QUERY_PER_KEY)], axis=0)
            k = turned(h0 + QUERY_PER_KEY)
            scores = lax.dot_general(
                k, q, (((1,), (1,)), ((), ())), preferred_element_type=F32
            )
            kept = scores[:img_most]
            for j in range(1, img_tile):
                kept = jnp.where(own_image == j, scores[j * img_most : (j + 1) * img_most], kept)
            kept = jnp.where(causal, kept * np.float32(HEAD_SIZE ** (-0.5)), -1e30)
            weights = jnp.exp(kept - jnp.max(kept, axis=0, keepdims=True))
            probs = weights / row_sum(weights)
            seen += [probs[:, i * TILE : (i + 1) * TILE] for i in range(QUERY_PER_KEY)]
        probs_at[to, :] = jnp.concatenate(seen, axis=0).T.astype(BF16)

    def send_probs(c, first):
        for o in range((c * CHUNK + first) // block, (c * CHUNK + first + TILE) // block):
            copy_probs(o).start()


    pl.loop(0, slots_chunk, unroll=2)(pick)
    if chunks > 2:
        pl.loop(2 * slots_chunk, slots, unroll=2)(pick)
    pltpu.make_async_copy(w_proj, w1, w1_sem).wait()
    for j in range(2 * groups):
        w2_copy(j).start()
    project(0, 0, tiles1)
    send(0)
    tiles = CHUNK // TILE
    for c in range(chunks):
        more = c + 1 < chunks
        if c == 0:
            if more:
                project(1, 0, tiles1 - 1)
            arrived(0)
            pltpu.make_async_copy(w_qkv, w2, w2_sem).wait()
            values(0, lambda: project(1, tiles1 - 1, tiles1) if more else None)
            send_values(0)
            if more:
                send(1)
            for j in range(len(qk_tiles)):
                qk(0, j)
        if c + 2 < chunks:
            project(c + 2, 0, tiles1)
        if more:
            arrived(c + 1)
            if c + 2 < chunks:
                send(c + 2)

            def beside():
                qk(c + 1, 0)
                for t in range(tiles):
                    attend(c, t * TILE)

            values(c + 1, beside)
            for t in range(tiles):
                send_probs(c, t * TILE)
            send_values(c + 1)
            for j in range(1, len(qk_tiles)):
                qk(c + 1, j)
        else:
            for t in range(tiles):
                attend(c, t * TILE)
                send_probs(c, t * TILE)

    for outbox, inbox, sems in (
        (values_at, box_values, values_sems),
        (probs_at, box_probs, probs_sems),
    ):
        exchange(senders - 1, outbox, inbox, sems).wait()
        landed = inbox.at[far_rows]
        pltpu.make_async_copy(landed, landed, sems.at[1]).wait()
    for copy in meta:
        copy.wait()
    sent = normed.at[pl.ds(pl.multiple_of(core * half, half), half)]
    pltpu.make_async_copy(sent, sent, norm_send).wait()
    for c in range(chunks):
        copy_squares(c).wait_send()
        copy_hidden(c).wait_send()
    for outbox, sems in ((values_at, values_sems), (probs_at, probs_sems)):
        left = outbox.at[far_rows]
        pltpu.make_async_copy(left, left, sems.at[0]).wait()


def place_kernel(heads, img_most, *refs):
    cols_in, rows_in, probs_in, values_in, out, meta_cols, meta_rows, box, placed, in_sem, out_sem = refs
    box_rows, prob_cols = probs_in.shape
    loads = [
        pltpu.make_async_copy(there, here, in_sem.at[i])
        for i, (there, here) in enumerate(
            [
                (cols_in, meta_cols),
                (rows_in, meta_rows),
                (probs_in, box.at[:, pl.ds(0, prob_cols)]),
                (values_in, box.at[:, pl.ds(prob_cols, values_in.shape[1])]),
            ]
        )
    ]
    for copy in loads:
        copy.start()
    for copy in loads:
        copy.wait()
    groups = heads // QUERY_PER_KEY
    w = HEAD_SIZE
    tiles = out.shape[0] // TILE

    def out_copy(t):
        at = pl.ds(t * TILE, TILE)
        return pltpu.make_async_copy(placed.at[at], out.at[at], out_sem.at[t])

    key_at = iota((heads * img_most, TILE), 0)
    ats = [slice(t * TILE, (t + 1) * TILE) for t in range(tiles)]
    slot_at = iota((TILE, box_rows), 1)
    selects = [jnp.where(slot_at == meta_cols[at, 0:1], 1.0, 0.0).astype(BF16) for at in ats]
    own = [
        jnp.dot(select, box[...], preferred_element_type=F32).astype(BF16) for select in selects
    ]
    expanded = []
    for t, at in enumerate(ats):
        inside = meta_rows[1:2, at]
        expand = jnp.concatenate(
            [jnp.where(key_at == h * img_most + inside, 1.0, 0.0).astype(BF16) for h in range(heads)],
            axis=1,
        )
        expanded.append(jnp.dot(own[t][:, :prob_cols], expand, preferred_element_type=F32))
    for t, at in enumerate(ats):
        same = meta_cols[at, 1:2] == meta_rows[0:1, at]
        for g in range(groups):
            seen = jnp.concatenate(
                [
                    jnp.where(same, expanded[t][:, h * TILE : (h + 1) * TILE], 0.0).astype(BF16)
                    for h in range(g * QUERY_PER_KEY, (g + 1) * QUERY_PER_KEY)
                ],
                axis=0,
            )
            values = own[t][:, prob_cols + g * w : prob_cols + (g + 1) * w]
            attended = jnp.dot(seen, values, preferred_element_type=F32).astype(BF16)
            for i in range(QUERY_PER_KEY):
                a = (g * QUERY_PER_KEY + i) * w
                placed[at, a : a + w] = attended[i * TILE : (i + 1) * TILE]
        if t % 2 == 1:
            out_copy(t - 1).start()
            out_copy(t).start()
    for t in range(tiles):
        out_copy(t).wait()


def local(
    patches, ln_gain, ln_bias, w_proj, proj_bias, rms_gain, w_qkv, image_counts, source_shift
):
    senders = lax.axis_size("dp")
    half, d_vit = patches.shape
    rows = 2 * half
    parts = half // 64
    half_cols = w_proj.shape[1]
    qkv_cols = w_qkv.shape[1]
    groups = qkv_cols // ((QUERY_PER_KEY + 2) * HEAD_SIZE)
    heads = groups * QUERY_PER_KEY
    out_cols = heads * HEAD_SIZE
    images = source_shift.shape[0]
    img_most = TILE // (images // (rows // TILE))
    pair_slots = (images + senders - 1) // senders
    box_rows = senders * pair_slots * img_most
    prob_cols, value_cols = heads * img_most, groups * HEAD_SIZE
    chunks = box_rows // CHUNK
    hbm = pl.BlockSpec(memory_space=pl.ANY)
    dma = pltpu.SemaphoreType.DMA
    smalls = (
        ln_gain,
        ln_bias,
        proj_bias,
        rms_gain,
        image_counts.T,
        source_shift,
        jnp.asarray(rotary_table(TILE + img_most)),
    )
    probs, values, cols, lines = pl.pallas_call(
        functools.partial(kernel, senders),
        out_shape=[
            jax.ShapeDtypeStruct((box_rows, prob_cols), BF16),
            jax.ShapeDtypeStruct((box_rows, value_cols), BF16),
            jax.ShapeDtypeStruct((rows, LANES), I32),
            jax.ShapeDtypeStruct((8, rows), I32),
        ],
        in_specs=[hbm] * 10,
        out_specs=[hbm] * 4,
        scratch_shapes=[
            *[pltpu.VMEM(x.shape, x.dtype) for x in smalls],
            pltpu.VMEM((half, d_vit), BF16),
            pltpu.VMEM(w_proj.shape, BF16),
            pltpu.VMEM(w_qkv.shape, BF16),
            pltpu.VMEM((rows, d_vit), BF16),
            pltpu.VMEM(((rows + img_most) * (d_vit // LANES), LANES), F32),
            pltpu.VMEM((box_rows, d_vit), BF16),
            pltpu.VMEM((box_rows, 2 * half_cols), BF16),
            pltpu.VMEM((2, box_rows, LANES), F32),
            pltpu.VMEM((2, half_cols), F32),
            pltpu.VMEM((2, CHUNK, qkv_cols - value_cols), F32),
            pltpu.VMEM((box_rows, HEAD_SIZE), F32),
            pltpu.VMEM((box_rows, HEAD_SIZE), F32),
            pltpu.VMEM((box_rows, prob_cols), BF16),
            pltpu.VMEM((box_rows, value_cols), BF16),
            pltpu.VMEM((rows, LANES), I32),
            pltpu.VMEM((8, rows), I32),
            pltpu.VMEM((8, LANES), I32),
            pltpu.SMEM((8, LANES), I32),
            dma((len(smalls),)),
            dma((parts,)),
            dma,
            dma,
            dma,
            dma((2,)),
            dma,
            dma((parts,)),
            dma((chunks,)),
            dma((chunks,)),
            dma((chunks,)),
            dma((chunks,)),
            dma((3,)),
            dma((3,)),
        ],
        compiler_params=pltpu.CompilerParams(
            collective_id=0, has_side_effects=True, vmem_limit_bytes=60 * 1024 * 1024
        ),
        name="projector_attention",
    )(
        *smalls,
        patches,
        w_proj,
        w_qkv,
    )
    return pl.pallas_call(
        functools.partial(place_kernel, heads, img_most),
        out_shape=jax.ShapeDtypeStruct((rows, out_cols), BF16),
        in_specs=[hbm] * 4,
        out_specs=hbm,
        scratch_shapes=[
            pltpu.VMEM(cols.shape, I32),
            pltpu.VMEM(lines.shape, I32),
            pltpu.VMEM((box_rows, prob_cols + value_cols), BF16),
            pltpu.VMEM((rows, out_cols), BF16),
            dma((4,)),
            dma((rows // TILE,)),
        ],
        name="place",
    )(cols, lines, probs, values)


def solution(mesh):
    in_specs = (
        P(("dp", "mp"), None),
        P(),
        P(),
        P(None, "mp"),
        P("mp"),
        P(),
        P(None, "mp"),
        P(),
        P(),
    )
    out_specs = P("dp", "mp")
    return jax.shard_map(local, mesh=mesh, in_specs=in_specs, out_specs=out_specs, check_vma=False)
```
